32 devices in a mesh: gx: 2 (over x), gy: 4 (over y, core), gz: 4 (over z).
Axes of the slice: x: 2, y: 2, z: 4, core: 2. Of those that a mesh axis runs over, the one named last changes fastest.
Arguments:
- blocks: bfloat16 [512, 128, 1024], P(('gx', 'gy', 'gz')), may hold values from -0.375 to 0.375
- counts: int32 [512], P(('gx', 'gy', 'gz')), may hold values from 1 to 128
- owner: int32 [512, 1], P(('gx', 'gy', 'gz')), may hold values from 0 to 15; in each aligned block of 16 rows (0 to 15, 16 to 31, ...) no two rows name the same one
- kdiag: float32 [32, 1024], P(('gx', 'gy', 'gz')), may hold values from 0.5 to 4
- rhs: float32 [32, 1024], P(('gx', 'gy', 'gz')), may hold values from -40 to 40
- modes: float32 [32, 6, 1024], P(('gx', 'gy', 'gz')), may hold values from -6 to 6
Outputs:
- schur: bfloat16 [32, 1024, 1024], P(('gx', 'gy', 'gz'))
- solution: float32 [32, 1024], P(('gx', 'gy', 'gz'))
- residual: float32 [32, 1024], P(('gx', 'gy', 'gz'))
The draws below stay inside these ranges and needn't reach their ends.
Inputs may be any that keep to these rules, and one draw needn't show every extreme that they name: `owner`: the 16 blocks of one device go to different owners.
All inputs are finite; a program needn't handle non-finite values.
Results may differ from the reference program's by a relative error of at most 0.001.
Values may be sent and summed in bfloat16 or wider, within the bound.
A program may use at most 64 MiB of HBM per device.

```python
import math
import jax
import jax.numpy as jnp
import numpy as np
from jax import lax

NB = 1024
ROWS = 128
BLK_DEV = 16
NC = 6
ITERS = 2
SUBDOMAINS = 32
BLOCKS = 512
N_GX = 2
N_GY = 4
N_GZ = 4


def draw_rhs(key, part):
    index = jnp.arange(SUBDOMAINS, dtype=jnp.float32)[:, None]
    scale = 4.0 * (1.0 + 2.0 * index / max(SUBDOMAINS - 1, 1))
    values = jax.random.normal(jax.random.fold_in(key, 11), (SUBDOMAINS, NB), jnp.float32) * scale
    return jnp.clip(values, -40.0, 40.0)


def touch_ends(values, own_key, least, high):
    shape = values.shape
    place = [jax.random.randint(jax.random.fold_in(own_key, axis), (), 0, shape[axis]) for axis in range(len(shape))]
    values = values.at[tuple(place)].set(least)
    longest = shape.index(max(shape))
    place[longest] = (place[longest] + 1) % shape[longest]
    return values.at[tuple(place)].set(high)


def levels(rng, dims, cuts, low, top_value):
    def one(axis_at, parts):
        heights = jax.random.uniform(jax.random.fold_in(jax.random.fold_in(rng, 6), axis_at), (parts,), jnp.float32, low / len(cuts), top_value / len(cuts))
        return jnp.repeat(jnp.exp(heights), dims[axis_at] // parts).reshape((-1,) + (1,) * (len(dims) - axis_at - 1))

    factor_of = one(*cuts[0])
    for cut in cuts[1:]:
        factor_of = factor_of * one(*cut)
    return factor_of


def assign_block(stream_key, own, number, rows, count, top, limit, lean):
    ranking = jax.random.permutation(stream_key, count)
    crowded, ordinary = load_shares(count, rows * top, limit, lean, True), load_shares(count, rows * top, limit, lean, False)
    places = jnp.arange(count)

    def named(tallies, offset_by):
        used = int((tallies > 0).sum())
        fixed = max(1, used // 4)
        moved = fixed + (places - fixed + offset_by * (used - fixed)) % max(1, count - fixed)
        return jnp.zeros((count,), jnp.int32).at[ranking[jnp.where(places < fixed, places, moved)]].set(jnp.asarray(tallies, jnp.int32))

    tallies = jnp.where(number % 4 == 0, named(crowded, number // 4), named(ordinary, number - number // 4 - 1))
    mixed = jax.random.permutation(jax.random.fold_in(own, 3), count)
    donor, receiver = mixed[0:count // 2 * 2:2], mixed[1:count // 2 * 2:2]
    room = jnp.minimum(tallies[donor] - 1, limit - tallies[receiver]) // 2
    room = jnp.where((donor == ranking[0]) | (receiver == ranking[0]) | (tallies[receiver] == 0), 0, jnp.maximum(room, 0))
    moved = jax.random.randint(jax.random.fold_in(own, 4), (count // 2,), 0, 1 << 20) % (room + 1)
    tallies = tallies.at[donor].add(-moved).at[receiver].add(moved)
    labels = jnp.searchsorted(jnp.cumsum(tallies), jnp.arange(rows * top), side="right").astype(jnp.int32)
    table = labels.reshape(top, rows).T
    table = table[jax.random.permutation(jax.random.fold_in(own, 1), rows)]
    offset_by = jax.random.randint(jax.random.fold_in(own, 2), (rows, 1), 0, top)
    return jnp.take_along_axis(table, (jnp.arange(top)[None, :] + offset_by) % top, axis=1)


def load_shares(count, total, bound, slope, full):
    portions = [(1 << 20) // math.isqrt(rank ** slope) + 1 for rank in range(1, count + 1)]
    largest = bound if full else min(bound, max(-(-total // count), total * portions[0] // sum(portions)))
    least = 1 if total - largest >= count - 1 else 0
    given, surplus = [largest] + [least] * (count - 1), total - largest - least * (count - 1)
    while surplus > 0:
        free = [i for i in range(1, count) if given[i] < largest] or [i for i in range(1, count) if given[i] < bound]
        pool, left = sum([portions[i] for i in free]), surplus
        for i in free:
            more = min(bound - given[i], max(1, left * portions[i] // pool), surplus)
            given[i] = given[i] + more
            surplus = surplus - more
    return np.array(given)


def noise(key, extent, scale, reach, cuts=(), kind=jnp.bfloat16):
    loudness = levels(key, extent, cuts, -0.22, 0.18) if cuts else 1.0
    array = jax.random.normal(key, extent, jnp.float32) * scale * loudness
    return jnp.minimum(jnp.maximum(array, -reach), reach).astype(kind)


def setup_inputs(seed: int = 0) -> dict:
    key_of = jax.random.split(jax.random.key(seed), 7)
    blocks = noise(key_of[0], (BLOCKS, ROWS, NB), 0.0625, 0.375, ((0, 32),))
    counts = touch_ends(jax.random.randint(key_of[1], (BLOCKS,), 1, ROWS + 1), jax.random.fold_in(key_of[1], 1), 1, ROWS).astype(jnp.int32)
    owner_keys = jax.random.split(jax.random.fold_in(key_of[2], 1), BLOCKS // BLK_DEV)
    owner_turns = jax.random.permutation(jax.random.fold_in(key_of[2], 3), BLOCKS // BLK_DEV)
    owner = jax.vmap(lambda own, number: assign_block(jax.random.fold_in(key_of[2], 2), own, number, BLK_DEV, N_GY * N_GZ, 1, 1, 2))(owner_keys, owner_turns).reshape((BLOCKS, 1))
    kdiag = jnp.clip(jnp.exp(math.log(4.0) - 2.0794415 * jax.random.uniform(key_of[3], (SUBDOMAINS, NB), jnp.float32) ** levels(key_of[3], (SUBDOMAINS, NB), ((0, 32),), -0.2, 0.2)), 0.5, 4.0)
    rhs = draw_rhs(jax.random.fold_in(key_of[6], 71), 0)
    modes = noise(key_of[5], (SUBDOMAINS, NC, NB), 1.0, 6.0, ((0, 32),), jnp.float32)
    return dict(blocks=blocks, counts=counts, owner=owner, kdiag=kdiag, rhs=rhs, modes=modes)


def assemble(values):
    count = values.shape[1]
    width = values.shape[2]
    face = width // 8
    grid = values.reshape(N_GX, N_GY, N_GZ, count, width)
    next_x = jnp.roll(grid, -1, axis=0)
    prev_x = jnp.roll(grid, 1, axis=0)
    next_y = jnp.roll(grid, -1, axis=1)
    prev_y = jnp.roll(grid, 1, axis=1)
    next_z = jnp.roll(grid, -1, axis=2)
    prev_z = jnp.roll(grid, 1, axis=2)
    extra = jnp.concatenate([next_x[..., face:2 * face], prev_x[..., 0:face], next_y[..., 3 * face:4 * face], prev_y[..., 2 * face:3 * face], next_z[..., 6 * face:8 * face], prev_z[..., 4 * face:6 * face]], axis=-1)
    return (grid + extra).reshape(values.shape)

def reference(blocks, counts, owner, kdiag, rhs, modes):
    hi = lax.Precision.HIGHEST
    rowid = jnp.arange(ROWS, dtype=jnp.int32)[None, :, None]
    live = jnp.where(rowid < counts[:, None, None], blocks, jnp.zeros_like(blocks)).astype(jnp.float32)
    group = N_GY * N_GZ
    reader = jnp.arange(BLOCKS, dtype=jnp.int32) // BLK_DEV
    target = (reader // group * group + owner[:, 0]).astype(jnp.int32)
    start = jnp.eye(NB, dtype=jnp.float32)[None, :, :] * kdiag[:, :, None]

    def add_block(total, item):
        piece, where = item
        gram = jnp.dot(piece.T, piece, precision=hi)
        return (total.at[where].add(gram), None)
    stiff, _ = lax.scan(add_block, start, (live, target))
    schur = stiff.astype(jnp.bfloat16)
    loaded = assemble(jnp.concatenate([rhs[:, None, :], modes], axis=1))
    force = loaded[:, 0]
    basis = loaded[:, 1:]
    coarse = 0.5 * jnp.einsum('dcn,den->ce', basis, basis, precision=hi)
    gforce = 0.5 * jnp.einsum('dcn,dn->c', basis, force, precision=hi)
    fnorm = 0.5 * jnp.sum(force * force)
    factor = jnp.linalg.cholesky(coarse)
    coef = jax.scipy.linalg.cho_solve((factor, True), gforce)
    residual = force - jnp.einsum('c,dcn->dn', coef, basis, precision=hi)
    norm_now = fnorm - jnp.dot(gforce, coef, precision=hi)
    direction = residual
    solution = jnp.zeros_like(force)
    for step in range(ITERS):
        local = jnp.einsum('dij,dj->di', stiff, direction, precision=hi)
        image = assemble(local[:, None, :])[:, 0]
        gimage = 0.5 * jnp.einsum('dcn,dn->c', basis, image, precision=hi)
        coef = jax.scipy.linalg.cho_solve((factor, True), gimage)
        along = image - jnp.einsum('c,dcn->dn', coef, basis, precision=hi)
        alpha = norm_now / (0.5 * jnp.sum(direction * along))
        solution = solution + alpha * direction
        residual = residual - alpha * along
        norm_next = 0.5 * jnp.sum(residual * residual)
        direction = residual + norm_next / norm_now * direction
        norm_now = norm_next
    return (schur, solution, residual)
```

```python
import functools

import jax
import jax.numpy as jnp
from jax import lax
from jax.experimental import pallas as pl
from jax.experimental.pallas import tpu as pltpu
from jax.sharding import PartitionSpec as P

MESH = pl.DeviceIdType.MESH
HI = lax.Precision.HIGHEST
F32 = jnp.float32
BF16 = jnp.bfloat16
I16 = jnp.int16
TILE = 128
TOP = 32767.0
UNROLL = 64


def kernel(
    nx, ny, nz,
    counts_ref, owner_ref, blocks_ref, kdiag_ref, rhs_ref, modes_ref,
    schur_ref, sol_ref, res_ref,
    blk, outgoing, arrived, pool, stiff, high, code_out, code_in, meta_out, meta_in,
    stack, ext0, loc, ext, slots,
    load_sem, schur_sem, bsend, psend, precv, brecv, csend, crecv, msend, mrecv,
    fsend, frecv, rsend, rrecv,
):
    n = nx * ny * nz
    quarter = nz // 4
    half = 2 * quarter
    nblk, nrows, width = blk.shape
    nc = modes_ref.shape[0]
    face = width // 8
    tiles = width // TILE
    folds = tiles // 2
    ix, iy, iz = lax.axis_index("gx"), lax.axis_index("gy"), lax.axis_index("gz")
    me = (ix * ny + iy) * nz + iz
    place = iy * nz + iz
    side = iz // half
    off = iz % half
    seat = iy * half + off
    outer = jnp.logical_or(iz < quarter, iz >= 3 * quarter)
    inner = jnp.logical_not(outer)
    mirror = (iz + half) % nz
    near_lo = jnp.where(side == 0, quarter, half)
    far_lo = jnp.where(side == 0, half, quarter)
    group = ny * quarter
    team = ny * half

    def coords(flat):
        return (flat // (ny * nz), (flat // nz) % ny, flat % nz)

    def each_peer(act):
        if n <= UNROLL:
            steps = [
                (dx, dy, dz)
                for dx in range(nx) for dy in range(ny) for dz in range(nz)
                if dx or dy or dz
            ]
            steps.sort(key=lambda s: -(s[0] + min(s[1], ny - s[1]) + s[2]))
            for dx, dy, dz in steps:
                act(((ix + dx) % nx, (iy + dy) % ny, (iz + dz) % nz))
        else:
            def one(k, carry):
                act(coords((me + k) % n))
                return carry

            lax.fori_loop(1, n, one, 0)

    load = pltpu.make_async_copy(blocks_ref, blk, load_sem)
    load.start()
    barrier = pltpu.get_barrier_semaphore()
    each_peer(
        lambda device: pl.semaphore_signal(
            barrier, inc=1, device_id=device, device_id_type=MESH
        )
    )
    stack[...] = jnp.zeros_like(stack)
    for i in range(nc):
        stack[i : i + 1, :] = modes_ref[i]
    stack[nc : nc + 1, :] = rhs_ref[...]
    pl.semaphore_wait(barrier, n - 1)

    next_x, prev_x = ((ix + 1) % nx, iy, iz), ((ix + nx - 1) % nx, iy, iz)
    next_y, prev_y = (ix, (iy + 1) % ny, iz), (ix, (iy + ny - 1) % ny, iz)
    next_z, prev_z = (ix, iy, (iz + 1) % nz), (ix, iy, (iz + nz - 1) % nz)
    plan = (
        (4, 6, 2, next_z), (6, 4, 2, prev_z),
        (2, 3, 1, next_y), (3, 2, 1, prev_y),
        (0, 1, 1, next_x), (1, 0, 1, prev_x),
    )

    def faces(src, dst, turn):
        for mine, theirs, wide, device in plan:
            pltpu.make_async_remote_copy(
                src_ref=src.at[:, mine * face : (mine + wide) * face],
                dst_ref=dst.at[:, theirs * face : (theirs + wide) * face],
                send_sem=fsend.at[turn],
                recv_sem=frecv.at[turn],
                device_id=device,
                device_id_type=MESH,
            ).start()
        return pltpu.make_async_remote_copy(
            src_ref=src, dst_ref=dst, send_sem=fsend.at[turn], recv_sem=frecv.at[turn],
            device_id=next_x, device_id_type=MESH,
        )

    def share(turn, row):
        slots[turn, me] = row
        each_peer(
            lambda device: pltpu.make_async_remote_copy(
                src_ref=slots.at[turn, me],
                dst_ref=slots.at[turn, me],
                send_sem=rsend.at[turn],
                recv_sem=rrecv.at[turn],
                device_id=device,
                device_id_type=MESH,
            ).start()
        )

    def all_rows(turn):
        return pltpu.make_async_remote_copy(
            src_ref=slots.at[turn, pl.ds(0, n - 1)],
            dst_ref=slots.at[turn, pl.ds(0, n - 1)],
            send_sem=rsend.at[turn],
            recv_sem=rrecv.at[turn],
            device_id=next_x,
            device_id_type=MESH,
        )

    def gathered(turn):
        all_rows(turn).wait_recv()
        return jnp.sum(slots[turn], axis=0)

    first = faces(stack, ext0, 0)
    load.wait()

    owned = [owner_ref[b] for b in range(nblk)]
    counted = [counts_ref[b] for b in range(nblk)]
    rowid = lax.broadcasted_iota(jnp.int32, (nrows, width), 0)

    def chosen(target):
        which = jnp.int32(0)
        count = jnp.int32(0)
        for b in range(nblk):
            same = owned[b] == target
            which = jnp.where(same, b, which)
            count = jnp.where(same, counted[b], count)
        value = blk[which]
        return jnp.where(rowid < count, value, jnp.zeros_like(value))

    def block_rows(spot):
        return pl.ds(pl.multiple_of(spot * nrows, nrows), nrows)

    def block_copy(slot, ty, tz, src):
        return pltpu.make_async_remote_copy(
            src_ref=outgoing.at[slot],
            dst_ref=arrived.at[block_rows(src), :],
            send_sem=bsend,
            recv_sem=brecv.at[src // 2],
            device_id=(ix, ty, tz),
            device_id_type=MESH,
        )

    def pool_copy(slot, ty, tz, src):
        return pltpu.make_async_remote_copy(
            src_ref=outgoing.at[slot],
            dst_ref=pool.at[block_rows(src), :],
            send_sem=bsend,
            recv_sem=precv,
            device_id=(ix, ty, tz),
            device_id_type=MESH,
        )

    def push_pool(t, carry):
        ty = (iy + t // quarter) % ny
        tz = near_lo + (off + t) % quarter
        value = chosen(ty * nz + (tz + half) % nz)
        itself = jnp.logical_and(ty == iy, tz == iz)

        @pl.when(itself)
        def _():
            pool[block_rows(seat), :] = value

        @pl.when(jnp.logical_not(itself))
        def _():
            outgoing[t] = value
            pool_copy(t, ty, tz, seat).start()

        return carry

    def push_far(t, carry):
        ty = (iy + t // quarter) % ny
        tz = far_lo + (off + t) % quarter
        outgoing[group + t] = chosen(ty * nz + tz)
        block_copy(group + t, ty, tz, place).start()
        return carry

    def push_own(t, carry):
        ty = (iy + (t + 1) // half) % ny
        tz = side * half + (off + t + 1) % half
        outgoing[2 * group + t] = chosen(ty * nz + tz)
        block_copy(2 * group + t, ty, tz, place).start()
        return carry

    def push_both(t, carry):
        push_far(t, carry)
        return push_pool(t, carry)

    @pl.when(outer)
    def _():
        lax.fori_loop(0, group, push_pool, 0)
        lax.fori_loop(0, quarter, push_far, 0)

    @pl.when(inner)
    def _():
        lax.fori_loop(0, group, push_both, 0)

    lane = lax.broadcasted_iota(jnp.int32, (8, 128), 1)
    sub = lax.broadcasted_iota(jnp.int32, (8, 128), 0)
    sub1 = lax.broadcasted_iota(jnp.int32, (8, 1), 0)
    lane1 = lax.broadcasted_iota(jnp.int32, (1, 128), 1)

    first.wait_recv()
    work = stack[...] + ext0[...]
    tall = jnp.concatenate([work] * 16, axis=0)
    pairs = 0.5 * lax.dot_general(
        work, tall, (((1,), (1,)), ((), ())), precision=HI, preferred_element_type=F32
    )
    share(0, jnp.sum(jnp.where(lane // 8 == sub, pairs, 0.0), axis=0, keepdims=True))
    lax.fori_loop(0, team - 1, push_own, 0)

    @pl.when(outer)
    def _():
        lax.fori_loop(quarter, group, push_far, 0)

    arrived[block_rows(place), :] = chosen(place)

    diag_r = lax.broadcasted_iota(jnp.int32, (TILE, width), 0)
    diag_c = lax.broadcasted_iota(jnp.int32, (TILE, width), 1)
    for r in range(tiles):
        stiff[r * TILE : (r + 1) * TILE, :] = jnp.where(
            diag_r + r * TILE == diag_c, kdiag_ref[...], 0.0
        )

    tile_r = lax.broadcasted_iota(jnp.int32, (TILE, TILE), 0)
    tile_c = lax.broadcasted_iota(jnp.int32, (TILE, TILE), 1)
    above, below, level = tile_r < tile_c, tile_r > tile_c, tile_r == tile_c

    def cols(k):
        return slice(k * TILE, (k + 1) * TILE)

    def code_copy(a):
        return pltpu.make_async_remote_copy(
            src_ref=code_out.at[a], dst_ref=code_in.at[a],
            send_sem=csend, recv_sem=crecv.at[a],
            device_id=(ix, iy, mirror), device_id_type=MESH,
        )

    def meta_copy(a):
        return pltpu.make_async_remote_copy(
            src_ref=meta_out.at[a], dst_ref=meta_in.at[a],
            send_sem=msend, recv_sem=mrecv.at[a],
            device_id=(ix, iy, mirror), device_id_type=MESH,
        )

    @pl.when(inner)
    def _():
        pltpu.make_async_remote_copy(
            src_ref=pool.at[pl.ds(0, (team - 1) * nrows), :],
            dst_ref=pool.at[pl.ds(0, (team - 1) * nrows), :],
            send_sem=psend, recv_sem=precv,
            device_id=(ix, iy, mirror), device_id_type=MESH,
        ).wait_recv()

        def strip(k):
            return lax.dot_general(
                pool[:, cols(k)], pool[:, k * TILE :], (((0,), (0,)), ((), ())),
                preferred_element_type=F32,
            )

        for a in range(folds):
            b = tiles - 1 - a
            upper, lower = strip(a), strip(b)
            at_a, at_b = upper[:, :TILE], lower[:, :TILE]
            for k, corner in ((a, at_a), (b, at_b)):
                meta_out[folds, :, cols(k)] = jnp.sum(
                    jnp.where(level, corner, 0.0), axis=0, keepdims=True
                )
            corners = jnp.where(above, at_a, jnp.where(below, at_b, 0.0))
            parts = [upper[:, TILE:]]
            if a:
                parts.append(lower[:, TILE:])
            value = jnp.concatenate(parts + [corners], axis=1)
            most = jnp.max(jnp.abs(value), axis=0, keepdims=True)
            scale = TOP / jnp.maximum(most, 1e-30)
            code_out[a] = jnp.round(value * scale).astype(jnp.int32).astype(I16)
            meta_out[a] = most * (1.0 / TOP)
            code_copy(a).start()
            meta_copy(a).start()
        meta_copy(folds).start()

    def take(sy, sj):
        base = sy * nz + 2 * sj
        remote = pltpu.make_async_remote_copy(
            src_ref=outgoing.at[0],
            dst_ref=arrived.at[block_rows(base), :],
            send_sem=bsend, recv_sem=brecv.at[base // 2],
            device_id=(ix, iy, mirror), device_id_type=MESH,
        )
        pair = pl.ds(pl.multiple_of(base * nrows, 2 * nrows), 2 * nrows)
        both = pltpu.make_async_remote_copy(
            src_ref=arrived.at[pair, :], dst_ref=arrived.at[pair, :],
            send_sem=bsend, recv_sem=brecv.at[base // 2],
            device_id=(ix, iy, mirror), device_id_type=MESH,
        )
        mine = base // 2 == place // 2

        @pl.when(mine)
        def _():
            remote.wait_recv()

        @pl.when(jnp.logical_not(mine))
        def _():
            both.wait_recv()

        rows = arrived[pair, :]
        for c in range(width // 256):
            span = slice(c * 256, (c + 1) * 256)
            stiff[:, span] += lax.dot_general(
                rows, rows[:, span], (((0,), (0,)), ((), ())), preferred_element_type=F32
            )

    def take_own(u, carry):
        take((iy + ny - u // quarter) % ny, side * quarter + (off // 2 + u) % quarter)
        return carry

    def take_far(u, carry):
        take((iy + ny - u // quarter) % ny, (1 - side) * quarter + (off // 2 + u) % quarter)
        return carry

    lax.fori_loop(0, group, take_own, 0)

    @pl.when(outer)
    def _():
        for a in range(folds):
            b = tiles - 1 - a
            code_copy(a).wait_recv()
            meta_copy(a).wait_recv()
            value = code_in[a].astype(jnp.int32).astype(F32) * meta_in[a]
            spots = [(a, a + j) for j in range(1, tiles - a)]
            spots += [(b, b + j) for j in range(1, tiles - b)]
            for at, (r, c) in enumerate(spots):
                piece = value[:, cols(at)]
                stiff[cols(r), cols(c)] += piece
                stiff[cols(c), cols(r)] += piece.T
            corners = value[:, cols(tiles - 1)]
            turned = corners.T
            stiff[cols(a), cols(a)] += jnp.where(
                above, corners, jnp.where(below, turned, 0.0)
            )
            stiff[cols(b), cols(b)] += jnp.where(
                below, corners, jnp.where(above, turned, 0.0)
            )
        meta_copy(folds).wait_recv()
        for r in range(tiles):
            stiff[cols(r), cols(r)] += jnp.where(level, meta_in[folds, :, cols(r)], 0.0)

    total = gathered(0)
    spread = jnp.where(lane // 8 == sub, total, 0.0)
    fold_r = lax.broadcasted_iota(jnp.int32, (128, 128), 0)
    fold_c = lax.broadcasted_iota(jnp.int32, (128, 128), 1)
    fold = jnp.where(fold_r % 8 == fold_c, 1.0, 0.0).astype(F32)
    coarse = jnp.dot(spread, fold, precision=HI, preferred_element_type=F32)
    for k in range(nc):
        ratio = jnp.where(sub1 > k, coarse[:, k : k + 1] / coarse[k : k + 1, k : k + 1], 0.0)
        coarse_row = coarse[k : k + 1, :]
        work_row = work[k : k + 1, :]
        coarse = coarse - ratio * coarse_row
        work = work - ratio * work_row
    diag = jnp.sum(jnp.where(lane == sub, coarse, 0.0), axis=1, keepdims=True)
    norm_now = diag[nc : nc + 1, :]
    work = work * jnp.where(sub1 < nc, 1.0 / jnp.sqrt(jnp.where(sub1 < nc, diag, 1.0)), 1.0)
    direction = work[nc : nc + 1, :]
    basis = jnp.where(sub1 < nc, work, 0.0)

    @pl.when(inner)
    def _():
        lax.fori_loop(0, group, take_far, 0)

    def apply(vector):
        sums = [jnp.zeros((8, TILE), F32) for _ in range(tiles)]
        for k in range(tiles):
            column = jnp.broadcast_to(vector[:, cols(k)], (TILE, TILE)).T
            for c in range(tiles):
                product = stiff[cols(k), cols(c)] * column
                sums[c] = sums[c] + jnp.sum(product.reshape(TILE // 8, 8, TILE), axis=0)
        return jnp.concatenate([jnp.sum(s, axis=0, keepdims=True) for s in sums], axis=1)

    def as_row(column):
        return jnp.sum(jnp.where(lane == sub, column, 0.0), axis=0, keepdims=True)

    def as_column(row):
        return jnp.sum(jnp.where(lane == sub, row, 0.0), axis=1, keepdims=True)

    local = apply(direction)
    loc[0] = local
    second = faces(loc.at[0], ext.at[0], 1)
    share(1, as_row(jnp.sum(work * local, axis=1, keepdims=True)))
    for r in range(tiles):
        high[cols(r), :] = stiff[cols(r), :].astype(BF16)
    store = pltpu.make_async_copy(high, schur_ref.at[0], schur_sem)
    store.start()
    second.wait_recv()
    image = local + ext[0]
    g_one = as_column(gathered(1))
    curve_one = g_one[nc : nc + 1, :]
    alpha = norm_now / curve_one
    along = image - jnp.sum(g_one * basis, axis=0, keepdims=True)
    residual = direction - alpha * along
    answer = alpha * direction

    local = apply(residual)
    loc[1] = local
    third = faces(loc.at[1], ext.at[1], 2)
    probe = jnp.where(sub1 == nc + 1, residual, work)
    square = 0.5 * jnp.sum(residual * residual, axis=1, keepdims=True)
    row = as_row(jnp.sum(probe * local, axis=1, keepdims=True))
    share(2, jnp.where(lane1 == 8, square, row))
    third.wait_recv()
    total = gathered(2)
    g_two = as_column(total)
    norm_next = jnp.sum(jnp.where(lane1 == 8, total, 0.0), axis=1, keepdims=True)
    beta = norm_next / norm_now
    curve = (
        g_two[nc + 1 : nc + 2, :]
        + 2.0 * beta * g_two[nc : nc + 1, :]
        + beta * beta * curve_one
    )
    image = local + ext[1] + beta * image
    along = image - jnp.sum((g_two + beta * g_one) * basis, axis=0, keepdims=True)
    alpha = norm_next / curve
    sol_ref[...] = answer + alpha * (residual + beta * direction)
    res_ref[...] = residual - alpha * along

    for copies in (first, second, third):
        copies.wait_send()
    for turn in range(3):
        all_rows(turn).wait_send()

    def drained(count):
        whole = outgoing.at[pl.ds(0, count)]
        pltpu.make_async_remote_copy(
            src_ref=whole, dst_ref=whole, send_sem=bsend, recv_sem=precv,
            device_id=(ix, iy, mirror), device_id_type=MESH,
        ).wait_send()

    @pl.when(outer)
    def _():
        drained(2 * group + team - 1)

    @pl.when(inner)
    def _():
        drained(2 * group + team - 2)
        pltpu.make_async_remote_copy(
            src_ref=code_out, dst_ref=code_in, send_sem=csend, recv_sem=crecv.at[0],
            device_id=(ix, iy, mirror), device_id_type=MESH,
        ).wait_send()
        pltpu.make_async_remote_copy(
            src_ref=meta_out, dst_ref=meta_in, send_sem=msend, recv_sem=mrecv.at[0],
            device_id=(ix, iy, mirror), device_id_type=MESH,
        ).wait_send()

    store.wait()


def finish(schur_in, sol_in, res_in, schur_ref, sol_ref, res_ref, held, in_sem, out_sem):
    parts = held.shape[0]
    rows = held.shape[1]
    loads, stores = [], []
    for i in range(parts):
        span = pl.ds(i * rows, rows)
        loads.append(pltpu.make_async_copy(schur_in.at[0, span], held.at[i], in_sem.at[i]))
        stores.append(pltpu.make_async_copy(held.at[i], schur_ref.at[0, span], out_sem.at[i]))
    for load in loads:
        load.start()
    sol_ref[...] = sol_in[...]
    res_ref[...] = res_in[...]
    for load, store in zip(loads, stores):
        load.wait()
        store.start()
    for store in stores:
        store.wait()


def solution(mesh):
    nx, ny, nz = mesh.shape["gx"], mesh.shape["gy"], mesh.shape["gz"]
    n, owners = nx * ny * nz, ny * nz
    assert nz % 4 == 0

    def shards(blocks, counts, owner, kdiag, rhs, modes):
        nblk, nrows, width = blocks.shape
        folds = width // TILE // 2
        vmem = pl.BlockSpec(memory_space=pltpu.VMEM)
        smem = pl.BlockSpec(memory_space=pltpu.SMEM)
        hbm = pl.BlockSpec(memory_space=pl.ANY)
        dma = pltpu.SemaphoreType.DMA
        made = pl.pallas_call(
            functools.partial(kernel, nx, ny, nz),
            out_shape=(
                jax.ShapeDtypeStruct((1, width, width), BF16),
                jax.ShapeDtypeStruct((1, width), F32),
                jax.ShapeDtypeStruct((1, width), F32),
            ),
            in_specs=[smem, smem, hbm, vmem, vmem, vmem],
            out_specs=(hbm, vmem, vmem),
            scratch_shapes=[
                pltpu.VMEM((nblk, nrows, width), BF16),
                pltpu.VMEM((owners, nrows, width), BF16),
                pltpu.VMEM((owners * nrows, width), BF16),
                pltpu.VMEM((owners // 2 * nrows, width), BF16),
                pltpu.VMEM((width, width), F32),
                pltpu.VMEM((width, width), BF16),
                pltpu.VMEM((folds, TILE, width), I16),
                pltpu.VMEM((folds, TILE, width), I16),
                pltpu.VMEM((folds + 1, 1, width), F32),
                pltpu.VMEM((folds + 1, 1, width), F32),
                pltpu.VMEM((8, width), F32),
                pltpu.VMEM((8, width), F32),
                pltpu.VMEM((2, 1, width), F32),
                pltpu.VMEM((2, 1, width), F32),
                pltpu.VMEM((3, n, 1, 128), F32),
                dma, dma, dma, dma, dma,
                dma((owners // 2,)),
                dma, dma((folds,)), dma, dma((folds + 1,)),
                dma((3,)), dma((3,)), dma((3,)), dma((3,)),
            ],
            compiler_params=pltpu.CompilerParams(
                collective_id=0, has_side_effects=True, vmem_limit_bytes=60000 * 1024
            ),
        )(counts, owner[:, 0], blocks, kdiag, rhs, jnp.transpose(modes, (1, 0, 2)))
        return pl.pallas_call(
            finish,
            out_shape=(
                jax.ShapeDtypeStruct((1, width, width), BF16),
                jax.ShapeDtypeStruct((1, width), F32),
                jax.ShapeDtypeStruct((1, width), F32),
            ),
            in_specs=[hbm, vmem, vmem],
            out_specs=(hbm, vmem, vmem),
            scratch_shapes=[
                pltpu.VMEM((8, width // 8, width), BF16),
                pltpu.SemaphoreType.DMA((8,)),
                pltpu.SemaphoreType.DMA((8,)),
            ],
        )(*made)

    every = ("gx", "gy", "gz")
    return jax.shard_map(
        shards,
        mesh=mesh,
        in_specs=(
            P(every, None, None), P(every), P(every, None),
            P(every, None), P(every, None), P(every, None, None),
        ),
        out_specs=(P(every, None, None), P(every, None), P(every, None)),
        check_vma=False,
    )
```

```python
import functools

import jax
import jax.numpy as jnp
from jax import lax
from jax.experimental import pallas as pl
from jax.experimental.pallas import tpu as pltpu
from jax.sharding import PartitionSpec as P

MESH = pl.DeviceIdType.MESH
HI = lax.Precision.HIGHEST
F32 = jnp.float32
BF16 = jnp.bfloat16
I16 = jnp.int16
TILE = 128
TOP = 32767.0
UNROLL = 64
PARTS = 8


def kernel(
    nx, ny, nz,
    counts_hbm, owner_hbm, blocks_ref, kdiag_hbm, rhs_hbm, modes_hbm,
    schur_ref, sol_ref, res_ref,
    counts_ref, owner_ref, kdiag_ref, rhs_ref, modes_ref, blk, outgoing, arrived, pool, passing, stiff, high, code_out, code_in, meta_out, meta_in,
    stack, ext0, loc, ext, slots,
    load_sem, small_sem, schur_sem, bsend, psend, precv, hop_send, hop_recv, brecv, csend, crecv, msend, mrecv,
    fsend, frecv, rsend, rrecv,
):
    n = nx * ny * nz
    quarter = nz // 4
    half = 2 * quarter
    nblk, nrows, width = blk.shape
    nc = modes_ref.shape[0]
    face = width // 8
    tiles = width // TILE
    folds = tiles // 2
    ix, iy, iz = lax.axis_index("gx"), lax.axis_index("gy"), lax.axis_index("gz")
    me = (ix * ny + iy) * nz + iz
    place = iy * nz + iz
    side = iz // half
    off = iz % half
    seat = iy * half + off
    outer = jnp.logical_or(iz < quarter, iz >= 3 * quarter)
    inner = jnp.logical_not(outer)
    mirror = (iz + half) % nz
    near_lo = jnp.where(side == 0, quarter, half)
    far_lo = jnp.where(side == 0, half, quarter)
    group = ny * quarter
    team = ny * half

    def coords(flat):
        return (flat // (ny * nz), (flat // nz) % ny, flat % nz)

    def each_peer(act):
        if n <= UNROLL:
            steps = [
                (dx, dy, dz)
                for dx in range(nx) for dy in range(ny) for dz in range(nz)
                if dx or dy or dz
            ]
            steps.sort(key=lambda s: -(s[0] + min(s[1], ny - s[1]) + s[2]))
            for dx, dy, dz in steps:
                act(((ix + dx) % nx, (iy + dy) % ny, (iz + dz) % nz))
        else:
            def one(k, carry):
                act(coords((me + k) % n))
                return carry

            lax.fori_loop(1, n, one, 0)

    barrier = pltpu.get_barrier_semaphore()
    for dy in range(ny):
        for dz in range(nz):
            if dy or dz:
                pl.semaphore_signal(
                    barrier, inc=1, device_id=(ix, (iy + dy) % ny, (iz + dz) % nz),
                    device_id_type=MESH,
                )
    pl.semaphore_signal(barrier, inc=1, device_id=((ix + 1) % nx, iy, iz), device_id_type=MESH)
    extra = 1
    if nx > 2:
        pl.semaphore_signal(
            barrier, inc=1, device_id=((ix + nx - 1) % nx, iy, iz), device_id_type=MESH
        )
        extra = 2
    smalls = [
        pltpu.make_async_copy(src, dst, small_sem.at[i])
        for i, (src, dst) in enumerate((
            (rhs_hbm, rhs_ref), (modes_hbm, modes_ref), (owner_hbm, owner_ref),
            (counts_hbm, counts_ref), (kdiag_hbm, kdiag_ref),
        ))
    ]
    for small in smalls:
        small.start()
    load = pltpu.make_async_copy(blocks_ref, blk, load_sem)
    load.start()
    stack[...] = jnp.zeros_like(stack)
    for small in smalls:
        small.wait()
    for i in range(nc):
        stack[i : i + 1, :] = modes_ref[i]
    stack[nc : nc + 1, :] = rhs_ref[...]
    pl.semaphore_wait(barrier, ny * nz - 1 + extra)

    next_x, prev_x = ((ix + 1) % nx, iy, iz), ((ix + nx - 1) % nx, iy, iz)
    next_y, prev_y = (ix, (iy + 1) % ny, iz), (ix, (iy + ny - 1) % ny, iz)
    next_z, prev_z = (ix, iy, (iz + 1) % nz), (ix, iy, (iz + nz - 1) % nz)
    plan = (
        (4, 6, 2, next_z), (6, 4, 2, prev_z),
        (2, 3, 1, next_y), (3, 2, 1, prev_y),
        (0, 1, 1, next_x), (1, 0, 1, prev_x),
    )

    def faces(src, dst, turn):
        for mine, theirs, wide, device in plan:
            pltpu.make_async_remote_copy(
                src_ref=src.at[:, mine * face : (mine + wide) * face],
                dst_ref=dst.at[:, theirs * face : (theirs + wide) * face],
                send_sem=fsend.at[turn],
                recv_sem=frecv.at[turn],
                device_id=device,
                device_id_type=MESH,
            ).start()
        return pltpu.make_async_remote_copy(
            src_ref=src, dst_ref=dst, send_sem=fsend.at[turn], recv_sem=frecv.at[turn],
            device_id=next_x, device_id_type=MESH,
        )

    def share(turn, row):
        slots[turn, me] = row
        each_peer(
            lambda device: pltpu.make_async_remote_copy(
                src_ref=slots.at[turn, me],
                dst_ref=slots.at[turn, me],
                send_sem=rsend.at[turn],
                recv_sem=rrecv.at[turn],
                device_id=device,
                device_id_type=MESH,
            ).start()
        )

    def all_rows(turn):
        return pltpu.make_async_remote_copy(
            src_ref=slots.at[turn, pl.ds(0, n - 1)],
            dst_ref=slots.at[turn, pl.ds(0, n - 1)],
            send_sem=rsend.at[turn],
            recv_sem=rrecv.at[turn],
            device_id=next_x,
            device_id_type=MESH,
        )

    def gathered(turn):
        all_rows(turn).wait_recv()
        return jnp.sum(slots[turn], axis=0)

    first = faces(stack, ext0, 0)
    load.wait()

    owned = [owner_ref[b] for b in range(nblk)]
    counted = [counts_ref[b] for b in range(nblk)]
    rowid = lax.broadcasted_iota(jnp.int32, (nrows, width), 0)

    def chosen(target):
        which = jnp.int32(0)
        count = jnp.int32(0)
        for b in range(nblk):
            same = owned[b] == target
            which = jnp.where(same, b, which)
            count = jnp.where(same, counted[b], count)
        value = blk[which]
        return jnp.where(rowid < count, value, jnp.zeros_like(value))

    def block_rows(spot):
        return pl.ds(pl.multiple_of(spot * nrows, nrows), nrows)

    def block_copy(slot, ty, tz, src):
        return pltpu.make_async_remote_copy(
            src_ref=outgoing.at[slot],
            dst_ref=arrived.at[block_rows(src), :],
            send_sem=bsend,
            recv_sem=brecv.at[src // 2],
            device_id=(ix, ty, tz),
            device_id_type=MESH,
        )

    def pool_copy(slot, ty, tz, src):
        return pltpu.make_async_remote_copy(
            src_ref=outgoing.at[slot],
            dst_ref=pool.at[block_rows(src), :],
            send_sem=bsend,
            recv_sem=precv,
            device_id=(ix, ty, tz),
            device_id_type=MESH,
        )

    def push_pool(t, carry):
        ty = (iy + t // quarter) % ny
        tz = near_lo + (off + t) % quarter
        value = chosen(ty * nz + (tz + half) % nz)
        itself = jnp.logical_and(ty == iy, tz == iz)

        @pl.when(itself)
        def _():
            pool[block_rows(seat), :] = value

        @pl.when(jnp.logical_not(itself))
        def _():
            outgoing[t] = value
            pool_copy(t, ty, tz, seat).start()

        return carry

    def push_far(t, carry):
        ty = (iy + t // quarter) % ny
        tz = far_lo + (off + t) % quarter
        outgoing[group + t] = chosen(ty * nz + tz)
        block_copy(group + t, ty, tz, place).start()
        return carry

    def push_own(t, carry):
        ty = (iy + (t + 1) // half) % ny
        tz = side * half + (off + t + 1) % half
        outgoing[2 * group + t] = chosen(ty * nz + tz)
        block_copy(2 * group + t, ty, tz, place).start()
        return carry

    def push_both(t, carry):
        push_far(t, carry)
        return push_pool(t, carry)

    def swing(u):
        return 2 * ((iy // 2 + u // 2) % (ny // 2)) + (iy + u) % 2

    direct = 2 * quarter
    hops = group - direct
    kinds = ((near_lo, half, 0), (near_lo, 0, 2 * group), (far_lo, 0, group))

    def fill(kind, t):
        lo, shift, slot = kinds[kind]
        ty, tz = swing(t // quarter), lo + (off + t) % quarter
        outgoing[slot + t] = chosen(ty * nz + (tz + shift) % nz)
        return slot + t, ty, tz

    def push_direct(kind):
        def one(t, carry):
            slot, ty, tz = fill(kind, t)
            if kind:
                block_copy(slot, ty, tz, place).start()
            else:
                pool_copy(slot, ty, tz, seat).start()
            return carry

        return one

    def hop_copy(slot, s, peer):
        return pltpu.make_async_remote_copy(
            src_ref=outgoing.at[slot], dst_ref=passing.at[s],
            send_sem=bsend, recv_sem=hop_recv.at[s],
            device_id=(ix, peer, iz), device_id_type=MESH,
        )

    def push_hop(kind):
        def one(s, carry):
            slot, ty, tz = fill(kind, direct + s)
            hop_copy(slot, kind * hops + s, 2 * (ty // 2) + iy % 2).start()
            return carry

        return one

    def pass_on(kind):
        def one(s, carry):
            t = direct + s
            turn = t // quarter // 2
            sy = 2 * ((iy // 2 + ny // 2 - turn) % (ny // 2)) + iy % 2
            ty = 2 * (iy // 2) + (iy + t // quarter) % 2
            tz = kinds[kind][0] + (off + t) % quarter
            hop_copy(0, kind * hops + s, iy).wait_recv()
            if kind:
                src = sy * nz + iz
                dst, sem = arrived.at[block_rows(src), :], brecv.at[src // 2]
            else:
                dst, sem = pool.at[block_rows(sy * half + off), :], precv
            pltpu.make_async_remote_copy(
                src_ref=passing.at[kind * hops + s], dst_ref=dst,
                send_sem=hop_send, recv_sem=sem,
                device_id=(ix, ty, tz), device_id_type=MESH,
            ).start()
            return carry

        return one

    out_lo = jnp.where(side == 0, 0, 3 * quarter)

    def push_out(t, carry):
        ty = (iy + (t + 1) // quarter) % ny
        tz = out_lo + (iz - out_lo + t + 1) % quarter
        outgoing[3 * group + t] = chosen(ty * nz + tz)
        block_copy(3 * group + t, ty, tz, place).start()
        return carry

    @pl.when(outer)
    def _():
        lax.fori_loop(0, quarter, push_direct(0), 0)
        lax.fori_loop(0, hops, push_hop(0), 0)
        lax.fori_loop(quarter, direct, push_direct(0), 0)
        lax.fori_loop(0, quarter, push_direct(2), 0)
        lax.fori_loop(0, hops, push_hop(1), 0)
        lax.fori_loop(0, hops, push_hop(2), 0)

    @pl.when(inner)
    def _():
        lax.fori_loop(0, group, push_both, 0)

    lane = lax.broadcasted_iota(jnp.int32, (8, 128), 1)
    sub = lax.broadcasted_iota(jnp.int32, (8, 128), 0)
    sub1 = lax.broadcasted_iota(jnp.int32, (8, 1), 0)
    lane1 = lax.broadcasted_iota(jnp.int32, (1, 128), 1)

    first.wait_recv()
    work = stack[...] + ext0[...]
    tall = jnp.concatenate([work] * 16, axis=0)
    pairs = 0.5 * lax.dot_general(
        work, tall, (((1,), (1,)), ((), ())), precision=HI, preferred_element_type=F32
    )
    share(0, jnp.sum(jnp.where(lane // 8 == sub, pairs, 0.0), axis=0, keepdims=True))

    @pl.when(inner)
    def _():
        lax.fori_loop(0, team - 1, push_own, 0)

    @pl.when(outer)
    def _():
        lax.fori_loop(0, group - 1, push_out, 0)
        lax.fori_loop(0, hops, pass_on(0), 0)
        lax.fori_loop(quarter, direct, push_direct(2), 0)
        lax.fori_loop(0, direct, push_direct(1), 0)
        lax.fori_loop(0, hops, pass_on(1), 0)
        lax.fori_loop(0, hops, pass_on(2), 0)

    arrived[block_rows(place), :] = chosen(place)

    diag_r = lax.broadcasted_iota(jnp.int32, (TILE, width), 0)
    diag_c = lax.broadcasted_iota(jnp.int32, (TILE, width), 1)
    for r in range(tiles):
        stiff[r * TILE : (r + 1) * TILE, :] = jnp.where(
            diag_r + r * TILE == diag_c, kdiag_ref[...], 0.0
        )

    tile_r = lax.broadcasted_iota(jnp.int32, (TILE, TILE), 0)
    tile_c = lax.broadcasted_iota(jnp.int32, (TILE, TILE), 1)
    above, below, level = tile_r < tile_c, tile_r > tile_c, tile_r == tile_c

    def cols(k):
        return slice(k * TILE, (k + 1) * TILE)

    def code_copy(a):
        return pltpu.make_async_remote_copy(
            src_ref=code_out.at[a], dst_ref=code_in.at[a],
            send_sem=csend, recv_sem=crecv.at[a],
            device_id=(ix, iy, mirror), device_id_type=MESH,
        )

    def meta_copy(a):
        return pltpu.make_async_remote_copy(
            src_ref=meta_out.at[a], dst_ref=meta_in.at[a],
            send_sem=msend, recv_sem=mrecv.at[a],
            device_id=(ix, iy, mirror), device_id_type=MESH,
        )

    @pl.when(inner)
    def _():
        pltpu.make_async_remote_copy(
            src_ref=pool.at[pl.ds(0, (team - 1) * nrows), :],
            dst_ref=pool.at[pl.ds(0, (team - 1) * nrows), :],
            send_sem=psend, recv_sem=precv,
            device_id=(ix, iy, mirror), device_id_type=MESH,
        ).wait_recv()

        def strip(k):
            return lax.dot_general(
                pool[:, cols(k)], pool[:, k * TILE :], (((0,), (0,)), ((), ())),
                preferred_element_type=F32,
            )

        for a in range(folds):
            b = tiles - 1 - a
            upper, lower = strip(a), strip(b)
            at_a, at_b = upper[:, :TILE], lower[:, :TILE]
            for k, corner in ((a, at_a), (b, at_b)):
                meta_out[folds, :, cols(k)] = jnp.sum(
                    jnp.where(level, corner, 0.0), axis=0, keepdims=True
                )
            corners = jnp.where(above, at_a, jnp.where(below, at_b, 0.0))
            parts = [upper[:, TILE:]]
            if a:
                parts.append(lower[:, TILE:])
            value = jnp.concatenate(parts + [corners], axis=1)
            most = jnp.max(jnp.abs(value), axis=0, keepdims=True)
            scale = TOP / jnp.maximum(most, 1e-30)
            code_out[a] = jnp.round(value * scale).astype(jnp.int32).astype(I16)
            meta_out[a] = most * (1.0 / TOP)
            code_copy(a).start()
            meta_copy(a).start()
        meta_copy(folds).start()

    def take(sy, sj):
        base = sy * nz + 2 * sj
        remote = pltpu.make_async_remote_copy(
            src_ref=outgoing.at[0],
            dst_ref=arrived.at[block_rows(base), :],
            send_sem=bsend, recv_sem=brecv.at[base // 2],
            device_id=(ix, iy, mirror), device_id_type=MESH,
        )
        pair = pl.ds(pl.multiple_of(base * nrows, 2 * nrows), 2 * nrows)
        both = pltpu.make_async_remote_copy(
            src_ref=arrived.at[pair, :], dst_ref=arrived.at[pair, :],
            send_sem=bsend, recv_sem=brecv.at[base // 2],
            device_id=(ix, iy, mirror), device_id_type=MESH,
        )
        mine = base // 2 == place // 2

        @pl.when(mine)
        def _():
            remote.wait_recv()

        @pl.when(jnp.logical_not(mine))
        def _():
            both.wait_recv()

        rows = arrived[pair, :]
        for c in range(width // 256):
            span = slice(c * 256, (c + 1) * 256)
            stiff[:, span] += lax.dot_general(
                rows, rows[:, span], (((0,), (0,)), ((), ())), preferred_element_type=F32
            )

    def take_own(u, carry):
        take(swing(u // quarter), side * quarter + (off // 2 + u) % quarter)
        return carry

    def take_far(u, carry):
        take(swing(u // quarter), (1 - side) * quarter + (off // 2 + u) % quarter)
        return carry

    @pl.when(inner)
    def _():
        lax.fori_loop(0, direct, take_far, 0)

    lax.fori_loop(0, group, take_own, 0)

    @pl.when(outer)
    def _():
        for a in range(folds):
            b = tiles - 1 - a
            code_copy(a).wait_recv()
            meta_copy(a).wait_recv()
            value = code_in[a].astype(jnp.int32).astype(F32) * meta_in[a]
            spots = [(a, a + j) for j in range(1, tiles - a)]
            spots += [(b, b + j) for j in range(1, tiles - b)]
            for at, (r, c) in enumerate(spots):
                piece = value[:, cols(at)]
                stiff[cols(r), cols(c)] += piece
                stiff[cols(c), cols(r)] += piece.T
            corners = value[:, cols(tiles - 1)]
            turned = corners.T
            stiff[cols(a), cols(a)] += jnp.where(
                above, corners, jnp.where(below, turned, 0.0)
            )
            stiff[cols(b), cols(b)] += jnp.where(
                below, corners, jnp.where(above, turned, 0.0)
            )
        meta_copy(folds).wait_recv()
        for r in range(tiles):
            stiff[cols(r), cols(r)] += jnp.where(level, meta_in[folds, :, cols(r)], 0.0)

    total = gathered(0)
    spread = jnp.where(lane // 8 == sub, total, 0.0)
    fold_r = lax.broadcasted_iota(jnp.int32, (128, 128), 0)
    fold_c = lax.broadcasted_iota(jnp.int32, (128, 128), 1)
    fold = jnp.where(fold_r % 8 == fold_c, 1.0, 0.0).astype(F32)
    coarse = jnp.dot(spread, fold, precision=HI, preferred_element_type=F32)
    for k in range(nc):
        ratio = jnp.where(sub1 > k, coarse[:, k : k + 1] / coarse[k : k + 1, k : k + 1], 0.0)
        coarse_row = coarse[k : k + 1, :]
        work_row = work[k : k + 1, :]
        coarse = coarse - ratio * coarse_row
        work = work - ratio * work_row
    diag = jnp.sum(jnp.where(lane == sub, coarse, 0.0), axis=1, keepdims=True)
    norm_now = diag[nc : nc + 1, :]
    work = work * jnp.where(sub1 < nc, 1.0 / jnp.sqrt(jnp.where(sub1 < nc, diag, 1.0)), 1.0)
    direction = work[nc : nc + 1, :]
    basis = jnp.where(sub1 < nc, work, 0.0)

    @pl.when(inner)
    def _():
        lax.fori_loop(direct, group, take_far, 0)

    def apply(vector):
        sums = [jnp.zeros((8, TILE), F32) for _ in range(tiles)]
        for k in range(tiles):
            column = jnp.broadcast_to(vector[:, cols(k)], (TILE, TILE)).T
            for c in range(tiles):
                product = stiff[cols(k), cols(c)] * column
                sums[c] = sums[c] + jnp.sum(product.reshape(TILE // 8, 8, TILE), axis=0)
        return jnp.concatenate([jnp.sum(s, axis=0, keepdims=True) for s in sums], axis=1)

    def as_row(column):
        return jnp.sum(jnp.where(lane == sub, column, 0.0), axis=0, keepdims=True)

    def as_column(row):
        return jnp.sum(jnp.where(lane == sub, row, 0.0), axis=1, keepdims=True)

    local = apply(direction)
    loc[0] = local
    second = faces(loc.at[0], ext.at[0], 1)
    share(1, as_row(jnp.sum(work * local, axis=1, keepdims=True)))
    for r in range(tiles):
        high[cols(r), :] = stiff[cols(r), :].astype(BF16)
    store = pltpu.make_async_copy(high, schur_ref.at[0], schur_sem)
    store.start()
    second.wait_recv()
    image = local + ext[0]
    g_one = as_column(gathered(1))
    curve_one = g_one[nc : nc + 1, :]
    alpha = norm_now / curve_one
    along = image - jnp.sum(g_one * basis, axis=0, keepdims=True)
    residual = direction - alpha * along
    answer = alpha * direction

    local = apply(residual)
    loc[1] = local
    third = faces(loc.at[1], ext.at[1], 2)
    probe = jnp.where(sub1 == nc + 1, residual, work)
    square = 0.5 * jnp.sum(residual * residual, axis=1, keepdims=True)
    row = as_row(jnp.sum(probe * local, axis=1, keepdims=True))
    share(2, jnp.where(lane1 == 8, square, row))
    third.wait_recv()
    total = gathered(2)
    g_two = as_column(total)
    norm_next = jnp.sum(jnp.where(lane1 == 8, total, 0.0), axis=1, keepdims=True)
    beta = norm_next / norm_now
    curve = (
        g_two[nc + 1 : nc + 2, :]
        + 2.0 * beta * g_two[nc : nc + 1, :]
        + beta * beta * curve_one
    )
    image = local + ext[1] + beta * image
    along = image - jnp.sum((g_two + beta * g_one) * basis, axis=0, keepdims=True)
    alpha = norm_next / curve
    sol_ref[...] = answer + alpha * (residual + beta * direction)
    res_ref[...] = residual - alpha * along

    for copies in (first, second, third):
        copies.wait_send()
    for turn in range(3):
        all_rows(turn).wait_send()

    def drained(count):
        whole = outgoing.at[pl.ds(0, count)]
        pltpu.make_async_remote_copy(
            src_ref=whole, dst_ref=whole, send_sem=bsend, recv_sem=precv,
            device_id=(ix, iy, mirror), device_id_type=MESH,
        ).wait_send()

    @pl.when(outer)
    def _():
        drained(4 * group - 1)
        pltpu.make_async_remote_copy(
            src_ref=passing, dst_ref=passing, send_sem=hop_send, recv_sem=hop_recv.at[0],
            device_id=(ix, iy, mirror), device_id_type=MESH,
        ).wait_send()

    @pl.when(inner)
    def _():
        drained(2 * group + team - 2)
        pltpu.make_async_remote_copy(
            src_ref=code_out, dst_ref=code_in, send_sem=csend, recv_sem=crecv.at[0],
            device_id=(ix, iy, mirror), device_id_type=MESH,
        ).wait_send()
        pltpu.make_async_remote_copy(
            src_ref=meta_out, dst_ref=meta_in, send_sem=msend, recv_sem=mrecv.at[0],
            device_id=(ix, iy, mirror), device_id_type=MESH,
        ).wait_send()

    store.wait()


def finish(schur_in, sol_in, res_in, schur_ref, sol_ref, res_ref, held, rows, in_sem, out_sem):
    parts = held.shape[0]
    size = held.shape[1]
    loads, stores = [], []
    for i in range(parts):
        span = pl.ds(i * size, size)
        loads.append(pltpu.make_async_copy(schur_in.at[0, span], held.at[i], in_sem.at[i]))
        stores.append(pltpu.make_async_copy(held.at[i], schur_ref.at[0, span], out_sem.at[i]))
    for i, (src, dst) in enumerate(((sol_in, sol_ref), (res_in, res_ref))):
        loads.append(pltpu.make_async_copy(src, rows.at[i], in_sem.at[parts + i]))
        stores.append(pltpu.make_async_copy(rows.at[i], dst, out_sem.at[parts + i]))
    for load in loads:
        load.start()
    for load, store in zip(loads, stores):
        load.wait()
        store.start()
    for store in stores:
        store.wait()


def solution(mesh):
    nx, ny, nz = mesh.shape["gx"], mesh.shape["gy"], mesh.shape["gz"]
    n, owners = nx * ny * nz, ny * nz
    assert nz % 4 == 0

    def shards(blocks, counts, owner, kdiag, rhs, modes):
        nblk, nrows, width = blocks.shape
        folds = width // TILE // 2
        hops = 3 * (ny - 2) * nz // 4
        vmem = pl.BlockSpec(memory_space=pltpu.VMEM)
        hbm = pl.BlockSpec(memory_space=pl.ANY)
        dma = pltpu.SemaphoreType.DMA
        made = pl.pallas_call(
            functools.partial(kernel, nx, ny, nz),
            out_shape=(
                jax.ShapeDtypeStruct((1, width, width), BF16),
                jax.ShapeDtypeStruct((1, width), F32),
                jax.ShapeDtypeStruct((1, width), F32),
            ),
            in_specs=[hbm] * 6,
            out_specs=(hbm, vmem, vmem),
            scratch_shapes=[
                pltpu.SMEM((nblk,), jnp.int32),
                pltpu.SMEM((nblk,), jnp.int32),
                pltpu.VMEM((1, width), F32),
                pltpu.VMEM((1, width), F32),
                pltpu.VMEM((modes.shape[1], 1, width), F32),
                pltpu.VMEM((nblk, nrows, width), BF16),
                pltpu.VMEM((owners, nrows, width), BF16),
                pltpu.VMEM((owners * nrows, width), BF16),
                pltpu.VMEM((owners // 2 * nrows, width), BF16),
                pltpu.VMEM((hops, nrows, width), BF16),
                pltpu.VMEM((width, width), F32),
                pltpu.VMEM((width, width), BF16),
                pltpu.VMEM((folds, TILE, width), I16),
                pltpu.VMEM((folds, TILE, width), I16),
                pltpu.VMEM((folds + 1, 1, width), F32),
                pltpu.VMEM((folds + 1, 1, width), F32),
                pltpu.VMEM((8, width), F32),
                pltpu.VMEM((8, width), F32),
                pltpu.VMEM((2, 1, width), F32),
                pltpu.VMEM((2, 1, width), F32),
                pltpu.VMEM((3, n, 1, 128), F32),
                dma, dma((5,)), dma, dma, dma, dma,
                dma, dma((hops,)),
                dma((owners // 2,)),
                dma, dma((folds,)), dma, dma((folds + 1,)),
                dma((3,)), dma((3,)), dma((3,)), dma((3,)),
            ],
            compiler_params=pltpu.CompilerParams(
                collective_id=0, has_side_effects=True, vmem_limit_bytes=60000 * 1024
            ),
        )(counts, owner[:, 0], blocks, kdiag, rhs, jnp.transpose(modes, (1, 0, 2)))
        return pl.pallas_call(
            finish,
            out_shape=(
                jax.ShapeDtypeStruct((1, width, width), BF16),
                jax.ShapeDtypeStruct((1, width), F32),
                jax.ShapeDtypeStruct((1, width), F32),
            ),
            in_specs=[hbm] * 3,
            out_specs=(hbm,) * 3,
            scratch_shapes=[
                pltpu.VMEM((PARTS, width // PARTS, width), BF16),
                pltpu.VMEM((2, 1, width), F32),
                pltpu.SemaphoreType.DMA((PARTS + 2,)),
                pltpu.SemaphoreType.DMA((PARTS + 2,)),
            ],
        )(*made)

    every = ("gx", "gy", "gz")
    return jax.shard_map(
        shards,
        mesh=mesh,
        in_specs=(
            P(every, None, None), P(every), P(every, None),
            P(every, None), P(every, None), P(every, None, None),
        ),
        out_specs=(P(every, None, None), P(every, None), P(every, None)),
        check_vma=False,
    )
```

```python
import functools

import jax
import jax.numpy as jnp
from jax import lax
from jax.experimental import pallas as pl
from jax.experimental.pallas import tpu as pltpu
from jax.sharding import PartitionSpec as P

MESH = pl.DeviceIdType.MESH
HI = lax.Precision.HIGHEST
F32 = jnp.float32
BF16 = jnp.bfloat16
I16 = jnp.int16
TILE = 128
TOP = 32767.0
UNROLL = 64
PARTS = 8


def kernel(
    nx, ny, nz,
    counts_hbm, owner_hbm, blocks_ref, kdiag_hbm, rhs_hbm, modes_hbm,
    schur_ref, sol_ref, res_ref,
    counts_ref, owner_ref, kdiag_ref, rhs_ref, modes_ref, blk, outgoing, arrived, pool, passing, stiff, high, code_out, code_in, meta_out, meta_in,
    probe_out, probe_in, part_out, part_in,
    stack, ext0, loc, ext, slots,
    y_sem, z_sem, load_sem, small_sem, schur_sem, bsend, psend, precv, hop_send, hop_recv, brecv, csend, crecv, msend, mrecv,
    probe_send, probe_recv, part_send, part_recv,
    fsend, frecv, rsend, rrecv,
):
    n = nx * ny * nz
    quarter = nz // 4
    half = 2 * quarter
    nblk, nrows, width = blk.shape
    nc = modes_ref.shape[0]
    face = width // 8
    tiles = width // TILE
    folds = tiles // 2
    ix, iy, iz = lax.axis_index("gx"), lax.axis_index("gy"), lax.axis_index("gz")
    me = (ix * ny + iy) * nz + iz
    place = iy * nz + iz
    spot = iz * ny + iy
    side = iz // half
    off = iz % half
    seat = iy * half + off
    outer = jnp.logical_or(iz < quarter, iz >= 3 * quarter)
    inner = jnp.logical_not(outer)
    mirror = (iz + half) % nz
    near_lo = jnp.where(side == 0, quarter, half)
    far_lo = jnp.where(side == 0, half, quarter)
    group = ny * quarter
    team = ny * half

    def coords(flat):
        return (flat // (ny * nz), (flat // nz) % ny, flat % nz)

    def each_peer(act):
        if n <= UNROLL:
            steps = [
                (dx, dy, dz)
                for dx in range(nx) for dy in range(ny) for dz in range(nz)
                if dx or dy or dz
            ]
            steps.sort(key=lambda s: -(s[0] + min(s[1], ny - s[1]) + s[2]))
            for dx, dy, dz in steps:
                act(((ix + dx) % nx, (iy + dy) % ny, (iz + dz) % nz))
        else:
            def one(k, carry):
                act(coords((me + k) % n))
                return carry

            lax.fori_loop(1, n, one, 0)

    barrier = pltpu.get_barrier_semaphore()
    x_line = [((ix + d) % nx, iy, iz) for d in range(1, nx)]
    y_line = [(ix, (iy + d) % ny, iz) for d in range(1, ny)]
    z_line = [(ix, iy, (iz + d) % nz) for d in range(1, nz)]

    def tell(sem, line):
        for device in line:
            pl.semaphore_signal(sem, inc=1, device_id=device, device_id_type=MESH)

    tell(barrier, z_line + y_line + x_line)
    smalls = [
        pltpu.make_async_copy(src, dst, small_sem.at[i])
        for i, (src, dst) in enumerate((
            (rhs_hbm, rhs_ref), (modes_hbm, modes_ref), (owner_hbm, owner_ref),
            (counts_hbm, counts_ref), (kdiag_hbm, kdiag_ref),
        ))
    ]
    for small in smalls:
        small.start()
    load = pltpu.make_async_copy(blocks_ref, blk, load_sem)
    load.start()
    stack[...] = jnp.zeros_like(stack)
    for small in smalls:
        small.wait()
    for i in range(nc):
        stack[i : i + 1, :] = modes_ref[i]
    stack[nc : nc + 1, :] = rhs_ref[...]
    pl.semaphore_wait(barrier, nx + ny + nz - 3)
    tell(y_sem, y_line)

    next_x, prev_x = ((ix + 1) % nx, iy, iz), ((ix + nx - 1) % nx, iy, iz)
    next_y, prev_y = (ix, (iy + 1) % ny, iz), (ix, (iy + ny - 1) % ny, iz)
    next_z, prev_z = (ix, iy, (iz + 1) % nz), (ix, iy, (iz + nz - 1) % nz)
    plan = (
        (4, 6, 2, next_z), (6, 4, 2, prev_z),
        (2, 3, 1, next_y), (3, 2, 1, prev_y),
        (0, 1, 1, next_x), (1, 0, 1, prev_x),
    )

    def faces(src, dst, turn):
        for mine, theirs, wide, device in plan:
            pltpu.make_async_remote_copy(
                src_ref=src.at[:, mine * face : (mine + wide) * face],
                dst_ref=dst.at[:, theirs * face : (theirs + wide) * face],
                send_sem=fsend.at[turn],
                recv_sem=frecv.at[turn],
                device_id=device,
                device_id_type=MESH,
            ).start()
        return pltpu.make_async_remote_copy(
            src_ref=src, dst_ref=dst, send_sem=fsend.at[turn], recv_sem=frecv.at[turn],
            device_id=next_x, device_id_type=MESH,
        )

    def share(turn, row):
        slots[turn, me] = row
        each_peer(
            lambda device: pltpu.make_async_remote_copy(
                src_ref=slots.at[turn, me],
                dst_ref=slots.at[turn, me],
                send_sem=rsend.at[turn],
                recv_sem=rrecv.at[turn],
                device_id=device,
                device_id_type=MESH,
            ).start()
        )

    def all_rows(turn):
        return pltpu.make_async_remote_copy(
            src_ref=slots.at[turn, pl.ds(0, n - 1)],
            dst_ref=slots.at[turn, pl.ds(0, n - 1)],
            send_sem=rsend.at[turn],
            recv_sem=rrecv.at[turn],
            device_id=next_x,
            device_id_type=MESH,
        )

    def gathered(turn):
        all_rows(turn).wait_recv()
        return jnp.sum(slots[turn], axis=0)

    first = faces(stack, ext0, 0)
    load.wait()

    owned = [owner_ref[b] for b in range(nblk)]
    counted = [counts_ref[b] for b in range(nblk)]
    rowid = lax.broadcasted_iota(jnp.int32, (nrows, width), 0)

    def chosen(target):
        which = jnp.int32(0)
        count = jnp.int32(0)
        for b in range(nblk):
            same = owned[b] == target
            which = jnp.where(same, b, which)
            count = jnp.where(same, counted[b], count)
        value = blk[which]
        return jnp.where(rowid < count, value, jnp.zeros_like(value))

    def block_rows(at):
        return pl.ds(pl.multiple_of(at * nrows, nrows), nrows)

    def block_copy(slot, ty, tz, src):
        return pltpu.make_async_remote_copy(
            src_ref=outgoing.at[slot],
            dst_ref=arrived.at[block_rows(src), :],
            send_sem=bsend,
            recv_sem=brecv.at[src // 2],
            device_id=(ix, ty, tz),
            device_id_type=MESH,
        )

    def pool_copy(slot, ty, tz, src):
        return pltpu.make_async_remote_copy(
            src_ref=outgoing.at[slot],
            dst_ref=pool.at[block_rows(src), :],
            send_sem=bsend,
            recv_sem=precv,
            device_id=(ix, ty, tz),
            device_id_type=MESH,
        )

    def push_pool(t, carry):
        ty = (iy + t // quarter) % ny
        tz = near_lo + (off + t) % quarter
        value = chosen(ty * nz + (tz + half) % nz)
        itself = jnp.logical_and(ty == iy, tz == iz)

        @pl.when(itself)
        def _():
            pool[block_rows(seat), :] = value

        @pl.when(jnp.logical_not(itself))
        def _():
            outgoing[t] = value
            pool_copy(t, ty, tz, seat).start()

        return carry

    def push_far(t, carry):
        ty = (iy + t // quarter) % ny
        tz = far_lo + (off + t) % quarter
        outgoing[group + t] = chosen(ty * nz + tz)
        block_copy(group + t, ty, tz, spot).start()
        return carry

    def push_own(t, carry):
        ty = (iy + (t + 1) // half) % ny
        tz = side * half + (off + t + 1) % half
        outgoing[2 * group + t] = chosen(ty * nz + tz)
        block_copy(2 * group + t, ty, tz, spot).start()
        return carry

    def push_both(t, carry):
        push_far(t, carry)
        return push_pool(t, carry)

    def swing(u):
        return 2 * ((iy // 2 + u // 2) % (ny // 2)) + (iy + u) % 2

    direct = 2 * quarter
    hops = group - direct
    kinds = ((near_lo, half, 0), (near_lo, 0, 2 * group), (far_lo, 0, group))

    def fill(kind, t):
        lo, shift, slot = kinds[kind]
        ty, tz = swing(t // quarter), lo + (off + t) % quarter
        outgoing[slot + t] = chosen(ty * nz + (tz + shift) % nz)
        return slot + t, ty, tz

    def push_direct(kind):
        def one(t, carry):
            slot, ty, tz = fill(kind, t)
            if kind:
                block_copy(slot, ty, tz, spot).start()
            else:
                pool_copy(slot, ty, tz, seat).start()
            return carry

        return one

    def hop_copy(slot, s, peer):
        return pltpu.make_async_remote_copy(
            src_ref=outgoing.at[slot], dst_ref=passing.at[s],
            send_sem=bsend, recv_sem=hop_recv.at[s],
            device_id=(ix, peer, iz), device_id_type=MESH,
        )

    def push_hop(kind):
        def one(s, carry):
            slot, ty, tz = fill(kind, direct + s)
            hop_copy(slot, kind * hops + s, 2 * (ty // 2) + iy % 2).start()
            return carry

        return one

    def pass_on(kind):
        def one(s, carry):
            t = direct + s
            turn = t // quarter // 2
            sy = 2 * ((iy // 2 + ny // 2 - turn) % (ny // 2)) + iy % 2
            ty = 2 * (iy // 2) + (iy + t // quarter) % 2
            tz = kinds[kind][0] + (off + t) % quarter
            if kind:
                src = iz * ny + sy
                dst, sem = arrived.at[block_rows(src), :], brecv.at[src // 2]
            else:
                hop_copy(0, s, iy).wait_recv()
                dst, sem = pool.at[block_rows(sy * half + off), :], precv
            pltpu.make_async_remote_copy(
                src_ref=passing.at[kind * hops + s], dst_ref=dst,
                send_sem=hop_send, recv_sem=sem,
                device_id=(ix, ty, tz), device_id_type=MESH,
            ).start()
            return carry

        return one

    out_lo = jnp.where(side == 0, 0, 3 * quarter)
    out_near, out_far = out_lo, 3 * quarter - out_lo
    mine_lo = near_lo

    def push_out(t, carry):
        ty = (iy + (t + 1) // quarter) % ny
        tz = out_lo + (iz - out_lo + t + 1) % quarter
        outgoing[3 * group + t] = chosen(ty * nz + tz)
        block_copy(3 * group + t, ty, tz, spot).start()
        return carry

    @pl.when(outer)
    def _():
        lax.fori_loop(0, quarter, push_direct(0), 0)
        lax.fori_loop(0, hops, push_hop(0), 0)

    @pl.when(inner)
    def _():
        lax.fori_loop(0, quarter, push_both, 0)

    lane = lax.broadcasted_iota(jnp.int32, (8, 128), 1)
    sub = lax.broadcasted_iota(jnp.int32, (8, 128), 0)
    sub1 = lax.broadcasted_iota(jnp.int32, (8, 1), 0)
    lane1 = lax.broadcasted_iota(jnp.int32, (1, 128), 1)

    pl.semaphore_wait(y_sem, ny - 1)
    tell(z_sem, z_line)
    first.wait_recv()
    pl.semaphore_wait(z_sem, nz - 1)
    work = stack[...] + ext0[...]
    tall = jnp.concatenate([work] * 16, axis=0)
    pairs = 0.5 * lax.dot_general(
        work, tall, (((1,), (1,)), ((), ())), precision=HI, preferred_element_type=F32
    )
    share(0, jnp.sum(jnp.where(lane // 8 == sub, pairs, 0.0), axis=0, keepdims=True))

    @pl.when(inner)
    def _():
        lax.fori_loop(quarter, group, push_both, 0)
        lax.fori_loop(0, team - 1, push_own, 0)

    @pl.when(outer)
    def _():
        lax.fori_loop(quarter, direct, push_direct(0), 0)
        lax.fori_loop(0, quarter, push_direct(2), 0)
        lax.fori_loop(0, hops, push_hop(1), 0)
        lax.fori_loop(0, hops, push_hop(2), 0)
        lax.fori_loop(0, group - 1, push_out, 0)
        lax.fori_loop(0, hops, pass_on(0), 0)
        lax.fori_loop(quarter, direct, push_direct(2), 0)
        lax.fori_loop(0, direct, push_direct(1), 0)

    arrived[block_rows(spot), :] = chosen(place)

    diag_r = lax.broadcasted_iota(jnp.int32, (TILE, width), 0)
    diag_c = lax.broadcasted_iota(jnp.int32, (TILE, width), 1)
    for r in range(tiles):
        stiff[r * TILE : (r + 1) * TILE, :] = jnp.where(
            diag_r + r * TILE == diag_c, kdiag_ref[...], 0.0
        )

    tile_r = lax.broadcasted_iota(jnp.int32, (TILE, TILE), 0)
    tile_c = lax.broadcasted_iota(jnp.int32, (TILE, TILE), 1)
    above, below, level = tile_r < tile_c, tile_r > tile_c, tile_r == tile_c

    def cols(k):
        return slice(k * TILE, (k + 1) * TILE)

    def code_copy(a):
        return pltpu.make_async_remote_copy(
            src_ref=code_out.at[a], dst_ref=code_in.at[a],
            send_sem=csend, recv_sem=crecv.at[a],
            device_id=(ix, iy, mirror), device_id_type=MESH,
        )

    def meta_copy(a):
        return pltpu.make_async_remote_copy(
            src_ref=meta_out.at[a], dst_ref=meta_in.at[a],
            send_sem=msend, recv_sem=mrecv.at[a],
            device_id=(ix, iy, mirror), device_id_type=MESH,
        )

    total = gathered(0)
    spread = jnp.where(lane // 8 == sub, total, 0.0)
    fold_r = lax.broadcasted_iota(jnp.int32, (128, 128), 0)
    fold_c = lax.broadcasted_iota(jnp.int32, (128, 128), 1)
    fold = jnp.where(fold_r % 8 == fold_c, 1.0, 0.0).astype(F32)
    coarse = jnp.dot(spread, fold, precision=HI, preferred_element_type=F32)
    for k in range(nc):
        ratio = jnp.where(sub1 > k, coarse[:, k : k + 1] / coarse[k : k + 1, k : k + 1], 0.0)
        coarse_row = coarse[k : k + 1, :]
        work_row = work[k : k + 1, :]
        coarse = coarse - ratio * coarse_row
        work = work - ratio * work_row
    diag = jnp.sum(jnp.where(lane == sub, coarse, 0.0), axis=1, keepdims=True)
    norm_now = diag[nc : nc + 1, :]
    work = work * jnp.where(sub1 < nc, 1.0 / jnp.sqrt(jnp.where(sub1 < nc, diag, 1.0)), 1.0)
    direction = work[nc : nc + 1, :]
    basis = jnp.where(sub1 < nc, work, 0.0)

    probe_out[...] = direction
    late = 2 * hops

    def probe_copy(k, c, z):
        base, away = ((out_near, near_lo), (out_far, far_lo))[k]
        tz = base + z
        ty = 2 * (iy // 2) + c
        j = (iy + c) % 2
        far_off = tz % half
        r = (iz - mine_lo + quarter - far_off % quarter) % quarter
        return pltpu.make_async_remote_copy(
            src_ref=probe_out,
            dst_ref=probe_in.at[k * hops + j * quarter + r],
            send_sem=probe_send, recv_sem=probe_recv,
            device_id=(ix, ty, tz), device_id_type=MESH,
        )

    def whole(ref, send, recv):
        return pltpu.make_async_remote_copy(
            src_ref=ref, dst_ref=ref, send_sem=send, recv_sem=recv,
            device_id=(ix, iy, mirror), device_id_type=MESH,
        )

    sub16 = lax.broadcasted_iota(jnp.int32, (16, width), 0)
    sub16t = lax.broadcasted_iota(jnp.int32, (16, nrows), 0)

    def thirds(row, which):
        x = row.astype(BF16).astype(F32)
        y = (row - x).astype(BF16).astype(F32)
        z = row - x - y
        return jnp.where(
            which == 0, x, jnp.where(which == 1, y, jnp.where(which == 2, z, 0.0))
        ).astype(BF16)

    @pl.when(inner)
    def _():
        for k in range(2):
            for c in range(2):
                for z in range(quarter):
                    probe_copy(k, c, z).start()

    @pl.when(outer)
    def _():
        def landed(s, carry):
            hop_copy(0, hops + s, iy).wait_recv()
            return carry

        lax.fori_loop(0, late, landed, 0)
        whole(probe_in, probe_send, probe_recv).wait_recv()

        def part(s, carry):
            rows = passing[hops + s]
            inside = jnp.sum(lax.dot_general(
                thirds(probe_in[s], sub16), rows, (((1,), (1,)), ((), ())),
                preferred_element_type=F32,
            ), axis=0, keepdims=True)
            part_out[s] = jnp.sum(jnp.dot(
                thirds(inside, sub16t), rows, preferred_element_type=F32
            ), axis=0, keepdims=True)
            k = s // hops
            t = direct + s % hops
            j = t // quarter - 2
            tz = jnp.where(k == 0, near_lo, far_lo) + (off + t) % quarter
            pltpu.make_async_remote_copy(
                src_ref=part_out.at[s],
                dst_ref=part_in.at[k * hops + j * quarter + iz - out_lo],
                send_sem=part_send, recv_sem=part_recv,
                device_id=(ix, 2 * (iy // 2) + (iy + j) % 2, tz), device_id_type=MESH,
            ).start()
            return carry

        lax.fori_loop(0, late, part, 0)
        lax.fori_loop(0, hops, pass_on(1), 0)
        lax.fori_loop(0, quarter, pass_on(2), 0)

    @pl.when(inner)
    def _():
        pltpu.make_async_remote_copy(
            src_ref=pool.at[pl.ds(0, (team - 1) * nrows), :],
            dst_ref=pool.at[pl.ds(0, (team - 1) * nrows), :],
            send_sem=psend, recv_sem=precv,
            device_id=(ix, iy, mirror), device_id_type=MESH,
        ).wait_recv()

        def strip(k):
            return lax.dot_general(
                pool[:, cols(k)], pool[:, k * TILE :], (((0,), (0,)), ((), ())),
                preferred_element_type=F32,
            )

        for a in range(folds):
            b = tiles - 1 - a
            upper, lower = strip(a), strip(b)
            at_a, at_b = upper[:, :TILE], lower[:, :TILE]
            for k, corner in ((a, at_a), (b, at_b)):
                meta_out[folds, :, cols(k)] = jnp.sum(
                    jnp.where(level, corner, 0.0), axis=0, keepdims=True
                )
            corners = jnp.where(above, at_a, jnp.where(below, at_b, 0.0))
            parts = [upper[:, TILE:]]
            if a:
                parts.append(lower[:, TILE:])
            value = jnp.concatenate(parts + [corners], axis=1)
            most = jnp.max(jnp.abs(value), axis=0, keepdims=True)
            scale = TOP / jnp.maximum(most, 1e-30)
            code_out[a] = jnp.round(value * scale).astype(jnp.int32).astype(I16)
            meta_out[a] = most * (1.0 / TOP)
            code_copy(a).start()
            meta_copy(a).start()
        meta_copy(folds).start()

    def take(sz, chip):
        base = sz * ny + 2 * ((iy // 2 + chip) % (ny // 2))
        remote = pltpu.make_async_remote_copy(
            src_ref=outgoing.at[0],
            dst_ref=arrived.at[block_rows(base), :],
            send_sem=bsend, recv_sem=brecv.at[base // 2],
            device_id=(ix, iy, mirror), device_id_type=MESH,
        )
        pair = pl.ds(pl.multiple_of(base * nrows, 2 * nrows), 2 * nrows)
        both = pltpu.make_async_remote_copy(
            src_ref=arrived.at[pair, :], dst_ref=arrived.at[pair, :],
            send_sem=bsend, recv_sem=brecv.at[base // 2],
            device_id=(ix, iy, mirror), device_id_type=MESH,
        )
        mine = base // 2 == spot // 2

        @pl.when(mine)
        def _():
            remote.wait_recv()

        @pl.when(jnp.logical_not(mine))
        def _():
            both.wait_recv()

        rows = arrived[pair, :]
        for c in range(width // 256):
            span = slice(c * 256, (c + 1) * 256)
            stiff[:, span] += lax.dot_general(
                rows, rows[:, span], (((0,), (0,)), ((), ())), preferred_element_type=F32
            )

    chips = ny // 2

    def takes(lo, first_chip, last_chip):
        def one(u, carry):
            count = last_chip - first_chip
            take(lo + u // count, first_chip + u % count)
            return carry

        lax.fori_loop(0, quarter * (last_chip - first_chip), one, 0)

    @pl.when(inner)
    def _():
        takes(near_lo, 0, chips)
        takes(far_lo, 0, chips)
        takes(out_far, 0, 1)
        takes(out_near, 0, 1)

    @pl.when(outer)
    def _():
        takes(out_near, 0, chips)
        takes(near_lo, 0, chips)

    @pl.when(outer)
    def _():
        for a in range(folds):
            b = tiles - 1 - a
            code_copy(a).wait_recv()
            meta_copy(a).wait_recv()
            value = code_in[a].astype(jnp.int32).astype(F32) * meta_in[a]
            spots = [(a, a + j) for j in range(1, tiles - a)]
            spots += [(b, b + j) for j in range(1, tiles - b)]
            for at, (r, c) in enumerate(spots):
                piece = value[:, cols(at)]
                stiff[cols(r), cols(c)] += piece
                stiff[cols(c), cols(r)] += piece.T
            corners = value[:, cols(tiles - 1)]
            turned = corners.T
            stiff[cols(a), cols(a)] += jnp.where(
                above, corners, jnp.where(below, turned, 0.0)
            )
            stiff[cols(b), cols(b)] += jnp.where(
                below, corners, jnp.where(above, turned, 0.0)
            )
        meta_copy(folds).wait_recv()
        for r in range(tiles):
            stiff[cols(r), cols(r)] += jnp.where(level, meta_in[folds, :, cols(r)], 0.0)

    def apply(vector):
        sums = [jnp.zeros((8, TILE), F32) for _ in range(tiles)]
        for k in range(tiles):
            column = jnp.broadcast_to(vector[:, cols(k)], (TILE, TILE)).T
            for c in range(tiles):
                product = stiff[cols(k), cols(c)] * column
                sums[c] = sums[c] + jnp.sum(product.reshape(TILE // 8, 8, TILE), axis=0)
        return jnp.concatenate([jnp.sum(s, axis=0, keepdims=True) for s in sums], axis=1)

    def as_row(column):
        return jnp.sum(jnp.where(lane == sub, column, 0.0), axis=0, keepdims=True)

    def as_column(row):
        return jnp.sum(jnp.where(lane == sub, row, 0.0), axis=1, keepdims=True)

    local = apply(direction)
    loc[0] = local

    @pl.when(inner)
    def _():
        whole(part_in, part_send, part_recv).wait_recv()
        loc[0] = local + jnp.sum(part_in[...], axis=0)

    local = loc[0]
    second = faces(loc.at[0], ext.at[0], 1)
    share(1, as_row(jnp.sum(work * local, axis=1, keepdims=True)))

    @pl.when(outer)
    def _():
        lax.fori_loop(quarter, hops, pass_on(2), 0)

    @pl.when(inner)
    def _():
        takes(out_near, 1, chips)
        takes(out_far, 1, chips)

    second.wait_recv()
    image = local + ext[0]
    g_one = as_column(gathered(1))
    curve_one = g_one[nc : nc + 1, :]
    alpha = norm_now / curve_one
    along = image - jnp.sum(g_one * basis, axis=0, keepdims=True)
    residual = direction - alpha * along
    answer = alpha * direction

    local = apply(residual)
    loc[1] = local
    third = faces(loc.at[1], ext.at[1], 2)
    probe = jnp.where(sub1 == nc + 1, residual, work)
    square = 0.5 * jnp.sum(residual * residual, axis=1, keepdims=True)
    row = as_row(jnp.sum(probe * local, axis=1, keepdims=True))
    share(2, jnp.where(lane1 == 8, square, row))
    for r in range(tiles):
        high[cols(r), :] = stiff[cols(r), :].astype(BF16)
    store = pltpu.make_async_copy(high, schur_ref.at[0], schur_sem)
    store.start()
    third.wait_recv()
    total = gathered(2)
    g_two = as_column(total)
    norm_next = jnp.sum(jnp.where(lane1 == 8, total, 0.0), axis=1, keepdims=True)
    beta = norm_next / norm_now
    curve = (
        g_two[nc + 1 : nc + 2, :]
        + 2.0 * beta * g_two[nc : nc + 1, :]
        + beta * beta * curve_one
    )
    image = local + ext[1] + beta * image
    along = image - jnp.sum((g_two + beta * g_one) * basis, axis=0, keepdims=True)
    alpha = norm_next / curve
    sol_ref[...] = answer + alpha * (residual + beta * direction)
    res_ref[...] = residual - alpha * along

    for copies in (first, second, third):
        copies.wait_send()
    for turn in range(3):
        all_rows(turn).wait_send()

    def drained(count):
        whole = outgoing.at[pl.ds(0, count)]
        pltpu.make_async_remote_copy(
            src_ref=whole, dst_ref=whole, send_sem=bsend, recv_sem=precv,
            device_id=(ix, iy, mirror), device_id_type=MESH,
        ).wait_send()

    @pl.when(outer)
    def _():
        drained(4 * group - 1)
        whole(part_out, part_send, part_recv).wait_send()
        pltpu.make_async_remote_copy(
            src_ref=passing, dst_ref=passing, send_sem=hop_send, recv_sem=hop_recv.at[0],
            device_id=(ix, iy, mirror), device_id_type=MESH,
        ).wait_send()

    @pl.when(inner)
    def _():
        drained(2 * group + team - 2)
        whole(probe_in, probe_send, probe_recv).wait_send()
        pltpu.make_async_remote_copy(
            src_ref=code_out, dst_ref=code_in, send_sem=csend, recv_sem=crecv.at[0],
            device_id=(ix, iy, mirror), device_id_type=MESH,
        ).wait_send()
        pltpu.make_async_remote_copy(
            src_ref=meta_out, dst_ref=meta_in, send_sem=msend, recv_sem=mrecv.at[0],
            device_id=(ix, iy, mirror), device_id_type=MESH,
        ).wait_send()

    store.wait()


def finish(schur_in, sol_in, res_in, schur_ref, sol_ref, res_ref, held, rows, in_sem, out_sem):
    parts = held.shape[0]
    size = held.shape[1]
    loads, stores = [], []
    for i in range(parts):
        span = pl.ds(i * size, size)
        loads.append(pltpu.make_async_copy(schur_in.at[0, span], held.at[i], in_sem.at[i]))
        stores.append(pltpu.make_async_copy(held.at[i], schur_ref.at[0, span], out_sem.at[i]))
    for i, (src, dst) in enumerate(((sol_in, sol_ref), (res_in, res_ref))):
        loads.append(pltpu.make_async_copy(src, rows.at[i], in_sem.at[parts + i]))
        stores.append(pltpu.make_async_copy(rows.at[i], dst, out_sem.at[parts + i]))
    for load in loads:
        load.start()
    for load, store in zip(loads, stores):
        load.wait()
        store.start()
    for store in stores:
        store.wait()


def solution(mesh):
    nx, ny, nz = mesh.shape["gx"], mesh.shape["gy"], mesh.shape["gz"]
    n, owners = nx * ny * nz, ny * nz
    assert ny == 4 and nz % 4 == 0

    def shards(blocks, counts, owner, kdiag, rhs, modes):
        nblk, nrows, width = blocks.shape
        folds = width // TILE // 2
        late = 2 * (ny - 2) * nz // 4
        hops = late * 3 // 2
        vmem = pl.BlockSpec(memory_space=pltpu.VMEM)
        hbm = pl.BlockSpec(memory_space=pl.ANY)
        dma = pltpu.SemaphoreType.DMA
        made = pl.pallas_call(
            functools.partial(kernel, nx, ny, nz),
            out_shape=(
                jax.ShapeDtypeStruct((1, width, width), BF16),
                jax.ShapeDtypeStruct((1, width), F32),
                jax.ShapeDtypeStruct((1, width), F32),
            ),
            in_specs=[hbm] * 6,
            out_specs=(hbm, vmem, vmem),
            scratch_shapes=[
                pltpu.SMEM((nblk,), jnp.int32),
                pltpu.SMEM((nblk,), jnp.int32),
                pltpu.VMEM((1, width), F32),
                pltpu.VMEM((1, width), F32),
                pltpu.VMEM((modes.shape[1], 1, width), F32),
                pltpu.VMEM((nblk, nrows, width), BF16),
                pltpu.VMEM((owners, nrows, width), BF16),
                pltpu.VMEM((owners * nrows, width), BF16),
                pltpu.VMEM((owners // 2 * nrows, width), BF16),
                pltpu.VMEM((hops, nrows, width), BF16),
                pltpu.VMEM((width, width), F32),
                pltpu.VMEM((width, width), BF16),
                pltpu.VMEM((folds, TILE, width), I16),
                pltpu.VMEM((folds, TILE, width), I16),
                pltpu.VMEM((folds + 1, 1, width), F32),
                pltpu.VMEM((folds + 1, 1, width), F32),
                pltpu.VMEM((1, width), F32),
                pltpu.VMEM((late, 1, width), F32),
                pltpu.VMEM((late, 1, width), F32),
                pltpu.VMEM((late, 1, width), F32),
                pltpu.VMEM((8, width), F32),
                pltpu.VMEM((8, width), F32),
                pltpu.VMEM((2, 1, width), F32),
                pltpu.VMEM((2, 1, width), F32),
                pltpu.VMEM((3, n, 1, 128), F32),
                pltpu.SemaphoreType.REGULAR, pltpu.SemaphoreType.REGULAR,
                dma, dma((5,)), dma, dma, dma, dma,
                dma, dma((hops,)),
                dma((owners // 2,)),
                dma, dma((folds,)), dma, dma((folds + 1,)),
                dma, dma, dma, dma,
                dma((3,)), dma((3,)), dma((3,)), dma((3,)),
            ],
            compiler_params=pltpu.CompilerParams(
                collective_id=0, has_side_effects=True, vmem_limit_bytes=60000 * 1024
            ),
        )(counts, owner[:, 0], blocks, kdiag, rhs, jnp.transpose(modes, (1, 0, 2)))
        return pl.pallas_call(
            finish,
            out_shape=(
                jax.ShapeDtypeStruct((1, width, width), BF16),
                jax.ShapeDtypeStruct((1, width), F32),
                jax.ShapeDtypeStruct((1, width), F32),
            ),
            in_specs=[hbm] * 3,
            out_specs=(hbm,) * 3,
            scratch_shapes=[
                pltpu.VMEM((PARTS, width // PARTS, width), BF16),
                pltpu.VMEM((2, 1, width), F32),
                pltpu.SemaphoreType.DMA((PARTS + 2,)),
                pltpu.SemaphoreType.DMA((PARTS + 2,)),
            ],
        )(*made)

    every = ("gx", "gy", "gz")
    return jax.shard_map(
        shards,
        mesh=mesh,
        in_specs=(
            P(every, None, None), P(every), P(every, None),
            P(every, None), P(every, None), P(every, None, None),
        ),
        out_specs=(P(every, None, None), P(every, None), P(every, None)),
        check_vma=False,
    )
```

```python
import functools

import jax
import jax.numpy as jnp
from jax import lax
from jax.experimental import pallas as pl
from jax.experimental.pallas import tpu as pltpu
from jax.sharding import PartitionSpec as P

MESH = pl.DeviceIdType.MESH
HI = lax.Precision.HIGHEST
F32 = jnp.float32
BF16 = jnp.bfloat16
I16 = jnp.int16
TILE = 128
TOP = 32767.0
UNROLL = 64
PARTS = 8


def kernel(
    nx, ny, nz,
    counts_hbm, owner_hbm, blocks_ref, kdiag_hbm, rhs_hbm, modes_hbm,
    schur_ref, sol_ref, res_ref,
    counts_ref, owner_ref, kdiag_ref, rhs_ref, modes_ref, blk, outgoing, arrived, pool, passing, stiff, high, code_out, code_in, meta_out, meta_in,
    probe_out, probe_in, part_out, part_in,
    stack, ext0, loc, ext, slots, ends,
    y_sem, z_sem, load_sem, small_sem, schur_sem, bsend, psend, precv, hop_send, hop_recv, brecv, csend, crecv, msend, mrecv,
    probe_send, probe_recv, part_send, part_recv,
    fsend, frecv, rsend, rrecv, end_sem,
):
    n = nx * ny * nz
    quarter = nz // 4
    half = 2 * quarter
    nblk, nrows, width = blk.shape
    nc = modes_ref.shape[0]
    face = width // 8
    tiles = width // TILE
    folds = tiles // 2
    ix, iy, iz = lax.axis_index("gx"), lax.axis_index("gy"), lax.axis_index("gz")
    me = (ix * ny + iy) * nz + iz
    place = iy * nz + iz
    spot = iz * ny + iy
    side = iz // half
    off = iz % half
    seat = iy * half + off
    outer = jnp.logical_or(iz < quarter, iz >= 3 * quarter)
    inner = jnp.logical_not(outer)
    mirror = (iz + half) % nz
    near_lo = jnp.where(side == 0, quarter, half)
    far_lo = jnp.where(side == 0, half, quarter)
    group = ny * quarter
    team = ny * half

    def coords(flat):
        return (flat // (ny * nz), (flat // nz) % ny, flat % nz)

    def each_peer(act):
        if n <= UNROLL:
            steps = [
                (dx, dy, dz)
                for dx in range(nx) for dy in range(ny) for dz in range(nz)
                if dx or dy or dz
            ]
            steps.sort(key=lambda s: -(s[0] + min(s[1], ny - s[1]) + s[2]))
            for dx, dy, dz in steps:
                act(((ix + dx) % nx, (iy + dy) % ny, (iz + dz) % nz))
        else:
            def one(k, carry):
                act(coords((me + k) % n))
                return carry

            lax.fori_loop(1, n, one, 0)

    barrier = pltpu.get_barrier_semaphore()
    x_line = [((ix + d) % nx, iy, iz) for d in range(1, nx)]
    y_line = [(ix, (iy + d) % ny, iz) for d in range(1, ny)]
    z_line = [(ix, iy, (iz + d) % nz) for d in range(1, nz)]

    def tell(sem, line):
        for device in line:
            pl.semaphore_signal(sem, inc=1, device_id=device, device_id_type=MESH)

    tell(barrier, z_line + y_line + x_line)
    smalls = [
        pltpu.make_async_copy(src, dst, small_sem.at[i])
        for i, (src, dst) in enumerate((
            (rhs_hbm, rhs_ref), (modes_hbm, modes_ref), (owner_hbm, owner_ref),
            (counts_hbm, counts_ref), (kdiag_hbm, kdiag_ref),
        ))
    ]
    for small in smalls:
        small.start()
    load = pltpu.make_async_copy(blocks_ref, blk, load_sem)
    load.start()
    stack[...] = jnp.zeros_like(stack)
    for small in smalls:
        small.wait()
    for i in range(nc):
        stack[i : i + 1, :] = modes_ref[i]
    stack[nc : nc + 1, :] = rhs_ref[...]
    pl.semaphore_wait(barrier, nx + ny + nz - 3)
    tell(y_sem, y_line)

    next_x, prev_x = ((ix + 1) % nx, iy, iz), ((ix + nx - 1) % nx, iy, iz)
    next_y, prev_y = (ix, (iy + 1) % ny, iz), (ix, (iy + ny - 1) % ny, iz)
    next_z, prev_z = (ix, iy, (iz + 1) % nz), (ix, iy, (iz + nz - 1) % nz)
    plan = (
        (4, 6, 2, next_z), (6, 4, 2, prev_z),
        (2, 3, 1, next_y), (3, 2, 1, prev_y),
        (0, 1, 1, next_x), (1, 0, 1, prev_x),
    )

    def faces(src, dst, turn):
        for mine, theirs, wide, device in plan:
            pltpu.make_async_remote_copy(
                src_ref=src.at[:, mine * face : (mine + wide) * face],
                dst_ref=dst.at[:, theirs * face : (theirs + wide) * face],
                send_sem=fsend.at[turn],
                recv_sem=frecv.at[turn],
                device_id=device,
                device_id_type=MESH,
            ).start()
        return pltpu.make_async_remote_copy(
            src_ref=src, dst_ref=dst, send_sem=fsend.at[turn], recv_sem=frecv.at[turn],
            device_id=next_x, device_id_type=MESH,
        )

    def share(turn, row):
        slots[turn, me] = row
        each_peer(
            lambda device: pltpu.make_async_remote_copy(
                src_ref=slots.at[turn, me],
                dst_ref=slots.at[turn, me],
                send_sem=rsend.at[turn],
                recv_sem=rrecv.at[turn],
                device_id=device,
                device_id_type=MESH,
            ).start()
        )

    def all_rows(turn):
        return pltpu.make_async_remote_copy(
            src_ref=slots.at[turn, pl.ds(0, n - 1)],
            dst_ref=slots.at[turn, pl.ds(0, n - 1)],
            send_sem=rsend.at[turn],
            recv_sem=rrecv.at[turn],
            device_id=next_x,
            device_id_type=MESH,
        )

    def gathered(turn):
        all_rows(turn).wait_recv()
        return jnp.sum(slots[turn], axis=0)

    first = faces(stack, ext0, 0)
    load.wait()

    owned = [owner_ref[b] for b in range(nblk)]
    counted = [counts_ref[b] for b in range(nblk)]
    rowid = lax.broadcasted_iota(jnp.int32, (nrows, width), 0)

    def chosen(target):
        which = jnp.int32(0)
        count = jnp.int32(0)
        for b in range(nblk):
            same = owned[b] == target
            which = jnp.where(same, b, which)
            count = jnp.where(same, counted[b], count)
        value = blk[which]
        return jnp.where(rowid < count, value, jnp.zeros_like(value))

    def block_rows(at):
        return pl.ds(pl.multiple_of(at * nrows, nrows), nrows)

    def block_copy(slot, ty, tz, src):
        return pltpu.make_async_remote_copy(
            src_ref=outgoing.at[slot],
            dst_ref=arrived.at[block_rows(src), :],
            send_sem=bsend,
            recv_sem=brecv.at[src // 2],
            device_id=(ix, ty, tz),
            device_id_type=MESH,
        )

    def pool_copy(slot, ty, tz, src):
        return pltpu.make_async_remote_copy(
            src_ref=outgoing.at[slot],
            dst_ref=pool.at[block_rows(src), :],
            send_sem=bsend,
            recv_sem=precv,
            device_id=(ix, ty, tz),
            device_id_type=MESH,
        )

    def push_pool(t, carry):
        ty = (iy + t // quarter) % ny
        tz = near_lo + (off + t) % quarter
        value = chosen(ty * nz + (tz + half) % nz)
        itself = jnp.logical_and(ty == iy, tz == iz)

        @pl.when(itself)
        def _():
            pool[block_rows(seat), :] = value

        @pl.when(jnp.logical_not(itself))
        def _():
            outgoing[t] = value
            pool_copy(t, ty, tz, seat).start()

        return carry

    def push_far(t, carry):
        ty = (iy + t // quarter) % ny
        tz = far_lo + (off + t) % quarter
        outgoing[group + t] = chosen(ty * nz + tz)
        block_copy(group + t, ty, tz, spot).start()
        return carry

    def push_own(t, carry):
        ty = (iy + (t + 1) // half) % ny
        tz = side * half + (off + t + 1) % half
        outgoing[2 * group + t] = chosen(ty * nz + tz)
        block_copy(2 * group + t, ty, tz, spot).start()
        return carry

    def push_both(t, carry):
        push_far(t, carry)
        return push_pool(t, carry)

    def swing(u):
        return 2 * ((iy // 2 + u // 2) % (ny // 2)) + (iy + u) % 2

    direct = 2 * quarter
    hops = group - direct
    kinds = ((near_lo, half, 0), (near_lo, 0, 2 * group), (far_lo, 0, group))

    def fill(kind, t):
        lo, shift, slot = kinds[kind]
        ty, tz = swing(t // quarter), lo + (off + t) % quarter
        outgoing[slot + t] = chosen(ty * nz + (tz + shift) % nz)
        return slot + t, ty, tz

    def push_direct(kind):
        def one(t, carry):
            slot, ty, tz = fill(kind, t)
            if kind:
                block_copy(slot, ty, tz, spot).start()
            else:
                pool_copy(slot, ty, tz, seat).start()
            return carry

        return one

    def hop_copy(slot, s, peer):
        return pltpu.make_async_remote_copy(
            src_ref=outgoing.at[slot], dst_ref=passing.at[s],
            send_sem=bsend, recv_sem=hop_recv.at[s],
            device_id=(ix, peer, iz), device_id_type=MESH,
        )

    def push_hop(kind):
        def one(s, carry):
            slot, ty, tz = fill(kind, direct + s)
            hop_copy(slot, kind * hops + s, 2 * (ty // 2) + iy % 2).start()
            return carry

        return one

    def pass_on(kind):
        def one(s, carry):
            t = direct + s
            turn = t // quarter // 2
            sy = 2 * ((iy // 2 + ny // 2 - turn) % (ny // 2)) + iy % 2
            ty = 2 * (iy // 2) + (iy + t // quarter) % 2
            tz = kinds[kind][0] + (off + t) % quarter
            if kind:
                src = iz * ny + sy
                dst, sem = arrived.at[block_rows(src), :], brecv.at[src // 2]
            else:
                hop_copy(0, s, iy).wait_recv()
                dst, sem = pool.at[block_rows(sy * half + off), :], precv
            pltpu.make_async_remote_copy(
                src_ref=passing.at[kind * hops + s], dst_ref=dst,
                send_sem=hop_send, recv_sem=sem,
                device_id=(ix, ty, tz), device_id_type=MESH,
            ).start()
            return carry

        return one

    out_lo = jnp.where(side == 0, 0, 3 * quarter)
    out_near, out_far = out_lo, 3 * quarter - out_lo
    mine_lo = near_lo

    def push_out(t, carry):
        ty = (iy + (t + 1) // quarter) % ny
        tz = out_lo + (iz - out_lo + t + 1) % quarter
        outgoing[3 * group + t] = chosen(ty * nz + tz)
        block_copy(3 * group + t, ty, tz, spot).start()
        return carry

    @pl.when(outer)
    def _():
        lax.fori_loop(0, quarter, push_direct(0), 0)
        lax.fori_loop(0, hops, push_hop(0), 0)

    @pl.when(inner)
    def _():
        lax.fori_loop(0, quarter, push_both, 0)

    lane = lax.broadcasted_iota(jnp.int32, (8, 128), 1)
    sub = lax.broadcasted_iota(jnp.int32, (8, 128), 0)
    sub1 = lax.broadcasted_iota(jnp.int32, (8, 1), 0)
    lane1 = lax.broadcasted_iota(jnp.int32, (1, 128), 1)

    pl.semaphore_wait(y_sem, ny - 1)
    tell(z_sem, z_line)
    first.wait_recv()
    pl.semaphore_wait(z_sem, nz - 1)
    work = stack[...] + ext0[...]
    tall = jnp.concatenate([work] * 16, axis=0)
    pairs = 0.5 * lax.dot_general(
        work, tall, (((1,), (1,)), ((), ())), precision=HI, preferred_element_type=F32
    )
    share(0, jnp.sum(jnp.where(lane // 8 == sub, pairs, 0.0), axis=0, keepdims=True))

    @pl.when(inner)
    def _():
        lax.fori_loop(quarter, group, push_both, 0)
        lax.fori_loop(0, team - 1, push_own, 0)

    @pl.when(outer)
    def _():
        lax.fori_loop(quarter, direct, push_direct(0), 0)
        lax.fori_loop(0, hops, push_hop(1), 0)
        lax.fori_loop(0, hops, push_hop(2), 0)
        lax.fori_loop(0, group - 1, push_out, 0)
        lax.fori_loop(0, quarter, pass_on(0), 0)
        lax.fori_loop(quarter, direct, pass_on(0), 0)
        lax.fori_loop(0, quarter, push_direct(2), 0)
        lax.fori_loop(quarter, direct, push_direct(2), 0)
        lax.fori_loop(0, quarter, push_direct(1), 0)
        lax.fori_loop(quarter, direct, push_direct(1), 0)

    arrived[block_rows(spot), :] = chosen(place)

    diag_r = lax.broadcasted_iota(jnp.int32, (TILE, width), 0)
    diag_c = lax.broadcasted_iota(jnp.int32, (TILE, width), 1)
    for r in range(tiles):
        stiff[r * TILE : (r + 1) * TILE, :] = jnp.where(
            diag_r + r * TILE == diag_c, kdiag_ref[...], 0.0
        )

    tile_r = lax.broadcasted_iota(jnp.int32, (TILE, TILE), 0)
    tile_c = lax.broadcasted_iota(jnp.int32, (TILE, TILE), 1)
    above, below, level = tile_r < tile_c, tile_r > tile_c, tile_r == tile_c

    def cols(k):
        return slice(k * TILE, (k + 1) * TILE)

    def code_copy(a):
        return pltpu.make_async_remote_copy(
            src_ref=code_out.at[a], dst_ref=code_in.at[a],
            send_sem=csend, recv_sem=crecv.at[a],
            device_id=(ix, iy, mirror), device_id_type=MESH,
        )

    def meta_copy(a):
        return pltpu.make_async_remote_copy(
            src_ref=meta_out.at[a], dst_ref=meta_in.at[a],
            send_sem=msend, recv_sem=mrecv.at[a],
            device_id=(ix, iy, mirror), device_id_type=MESH,
        )

    total = gathered(0)
    spread = jnp.where(lane // 8 == sub, total, 0.0)
    fold_r = lax.broadcasted_iota(jnp.int32, (128, 128), 0)
    fold_c = lax.broadcasted_iota(jnp.int32, (128, 128), 1)
    fold = jnp.where(fold_r % 8 == fold_c, 1.0, 0.0).astype(F32)
    coarse = jnp.dot(spread, fold, precision=HI, preferred_element_type=F32)
    for k in range(nc):
        ratio = jnp.where(sub1 > k, coarse[:, k : k + 1] / coarse[k : k + 1, k : k + 1], 0.0)
        coarse_row = coarse[k : k + 1, :]
        work_row = work[k : k + 1, :]
        coarse = coarse - ratio * coarse_row
        work = work - ratio * work_row
    diag = jnp.sum(jnp.where(lane == sub, coarse, 0.0), axis=1, keepdims=True)
    norm_now = diag[nc : nc + 1, :]
    work = work * jnp.where(sub1 < nc, 1.0 / jnp.sqrt(jnp.where(sub1 < nc, diag, 1.0)), 1.0)
    direction = work[nc : nc + 1, :]
    basis = jnp.where(sub1 < nc, work, 0.0)

    probe_out[...] = direction
    late = 2 * hops

    def probe_copy(k, c, z):
        base, away = ((out_near, near_lo), (out_far, far_lo))[k]
        tz = base + z
        ty = 2 * (iy // 2) + c
        j = (iy + c) % 2
        far_off = tz % half
        r = (iz - mine_lo + quarter - far_off % quarter) % quarter
        return pltpu.make_async_remote_copy(
            src_ref=probe_out,
            dst_ref=probe_in.at[k * hops + j * quarter + r],
            send_sem=probe_send, recv_sem=probe_recv,
            device_id=(ix, ty, tz), device_id_type=MESH,
        )

    def whole(ref, send, recv):
        return pltpu.make_async_remote_copy(
            src_ref=ref, dst_ref=ref, send_sem=send, recv_sem=recv,
            device_id=(ix, iy, mirror), device_id_type=MESH,
        )

    sub16 = lax.broadcasted_iota(jnp.int32, (16, width), 0)
    sub16t = lax.broadcasted_iota(jnp.int32, (16, nrows), 0)

    def thirds(row, which):
        x = row.astype(BF16).astype(F32)
        y = (row - x).astype(BF16).astype(F32)
        z = row - x - y
        return jnp.where(
            which == 0, x, jnp.where(which == 1, y, jnp.where(which == 2, z, 0.0))
        ).astype(BF16)

    @pl.when(inner)
    def _():
        for k in range(2):
            for c in range(2):
                for z in range(quarter):
                    probe_copy(k, c, z).start()

    @pl.when(outer)
    def _():
        def landed(s, carry):
            hop_copy(0, hops + s, iy).wait_recv()
            return carry

        lax.fori_loop(0, late, landed, 0)
        whole(probe_in, probe_send, probe_recv).wait_recv()

        def part(s, carry):
            rows = passing[hops + s]
            inside = jnp.sum(lax.dot_general(
                thirds(probe_in[s], sub16), rows, (((1,), (1,)), ((), ())),
                preferred_element_type=F32,
            ), axis=0, keepdims=True)
            part_out[s] = jnp.sum(jnp.dot(
                thirds(inside, sub16t), rows, preferred_element_type=F32
            ), axis=0, keepdims=True)
            k = s // hops
            t = direct + s % hops
            j = t // quarter - 2
            tz = jnp.where(k == 0, near_lo, far_lo) + (off + t) % quarter
            pltpu.make_async_remote_copy(
                src_ref=part_out.at[s],
                dst_ref=part_in.at[k * hops + j * quarter + iz - out_lo],
                send_sem=part_send, recv_sem=part_recv,
                device_id=(ix, 2 * (iy // 2) + (iy + j) % 2, tz), device_id_type=MESH,
            ).start()
            return carry

        lax.fori_loop(0, late, part, 0)
        lax.fori_loop(0, hops, pass_on(1), 0)
        lax.fori_loop(0, quarter, pass_on(2), 0)

    @pl.when(inner)
    def _():
        pltpu.make_async_remote_copy(
            src_ref=pool.at[pl.ds(0, (team - 1) * nrows), :],
            dst_ref=pool.at[pl.ds(0, (team - 1) * nrows), :],
            send_sem=psend, recv_sem=precv,
            device_id=(ix, iy, mirror), device_id_type=MESH,
        ).wait_recv()

        def strip(k):
            return lax.dot_general(
                pool[:, cols(k)], pool[:, k * TILE :], (((0,), (0,)), ((), ())),
                preferred_element_type=F32,
            )

        for a in range(folds):
            b = tiles - 1 - a
            upper, lower = strip(a), strip(b)
            at_a, at_b = upper[:, :TILE], lower[:, :TILE]
            for k, corner in ((a, at_a), (b, at_b)):
                meta_out[folds, :, cols(k)] = jnp.sum(
                    jnp.where(level, corner, 0.0), axis=0, keepdims=True
                )
            corners = jnp.where(above, at_a, jnp.where(below, at_b, 0.0))
            parts = [upper[:, TILE:]]
            if a:
                parts.append(lower[:, TILE:])
            value = jnp.concatenate(parts + [corners], axis=1)
            most = jnp.max(jnp.abs(value), axis=0, keepdims=True)
            scale = TOP / jnp.maximum(most, 1e-30)
            code_out[a] = jnp.round(value * scale).astype(jnp.int32).astype(I16)
            meta_out[a] = most * (1.0 / TOP)
            code_copy(a).start()
            meta_copy(a).start()
        meta_copy(folds).start()

    def arrival(sz, chip):
        base = sz * ny + 2 * ((iy // 2 + chip) % (ny // 2))
        remote = pltpu.make_async_remote_copy(
            src_ref=outgoing.at[0],
            dst_ref=arrived.at[block_rows(base), :],
            send_sem=bsend, recv_sem=brecv.at[base // 2],
            device_id=(ix, iy, mirror), device_id_type=MESH,
        )
        pair = pl.ds(pl.multiple_of(base * nrows, 2 * nrows), 2 * nrows)
        both = pltpu.make_async_remote_copy(
            src_ref=arrived.at[pair, :], dst_ref=arrived.at[pair, :],
            send_sem=bsend, recv_sem=brecv.at[base // 2],
            device_id=(ix, iy, mirror), device_id_type=MESH,
        )
        mine = base // 2 == spot // 2

        @pl.when(mine)
        def _():
            remote.wait_recv()

        @pl.when(jnp.logical_not(mine))
        def _():
            both.wait_recv()

        return pair

    def add(pair):
        rows = arrived[pair, :]
        for c in range(width // 256):
            span = slice(c * 256, (c + 1) * 256)
            stiff[:, span] += lax.dot_general(
                rows, rows[:, span], (((0,), (0,)), ((), ())), preferred_element_type=F32
            )

    def take(sz, chip):
        add(arrival(sz, chip))

    chips = ny // 2

    def takes(lo, first_chip, last_chip):
        def one(u, carry):
            count = last_chip - first_chip
            take(lo + u // count, first_chip + u % count)
            return carry

        lax.fori_loop(0, quarter * (last_chip - first_chip), one, 0)

    @pl.when(inner)
    def _():
        takes(near_lo, 0, chips)
        takes(far_lo, 0, chips)
        takes(out_far, 0, 1)
        takes(out_near, 0, 1)

    @pl.when(outer)
    def _():
        takes(out_near, 0, chips)
        takes(near_lo, 0, chips)

    @pl.when(outer)
    def _():
        for a in range(folds):
            b = tiles - 1 - a
            code_copy(a).wait_recv()
            meta_copy(a).wait_recv()
            value = code_in[a].astype(jnp.int32).astype(F32) * meta_in[a]
            spots = [(a, a + j) for j in range(1, tiles - a)]
            spots += [(b, b + j) for j in range(1, tiles - b)]
            for at, (r, c) in enumerate(spots):
                piece = value[:, cols(at)]
                stiff[cols(r), cols(c)] += piece
                stiff[cols(c), cols(r)] += piece.T
            corners = value[:, cols(tiles - 1)]
            turned = corners.T
            stiff[cols(a), cols(a)] += jnp.where(
                above, corners, jnp.where(below, turned, 0.0)
            )
            stiff[cols(b), cols(b)] += jnp.where(
                below, corners, jnp.where(above, turned, 0.0)
            )
        meta_copy(folds).wait_recv()
        for r in range(tiles):
            stiff[cols(r), cols(r)] += jnp.where(level, meta_in[folds, :, cols(r)], 0.0)

    def apply(vector):
        sums = [jnp.zeros((8, TILE), F32) for _ in range(tiles)]
        for k in range(tiles):
            column = jnp.broadcast_to(vector[:, cols(k)], (TILE, TILE)).T
            for c in range(tiles):
                product = stiff[cols(k), cols(c)] * column
                sums[c] = sums[c] + jnp.sum(product.reshape(TILE // 8, 8, TILE), axis=0)
        return jnp.concatenate([jnp.sum(s, axis=0, keepdims=True) for s in sums], axis=1)

    def as_row(column):
        return jnp.sum(jnp.where(lane == sub, column, 0.0), axis=0, keepdims=True)

    def as_column(row):
        return jnp.sum(jnp.where(lane == sub, row, 0.0), axis=1, keepdims=True)

    local = apply(direction)
    loc[0] = local

    @pl.when(inner)
    def _():
        whole(part_in, part_send, part_recv).wait_recv()
        loc[0] = local + jnp.sum(part_in[...], axis=0)

    local = loc[0]
    share(1, as_row(jnp.sum(work * local, axis=1, keepdims=True)))
    second = faces(loc.at[0], ext.at[0], 1)

    @pl.when(outer)
    def _():
        lax.fori_loop(quarter, hops, pass_on(2), 0)

    @pl.when(inner)
    def _():
        takes(out_near, 1, chips)

    second.wait_recv()
    image = local + ext[0]
    g_one = as_column(gathered(1))
    curve_one = g_one[nc : nc + 1, :]
    alpha = norm_now / curve_one
    along = image - jnp.sum(g_one * basis, axis=0, keepdims=True)
    residual = direction - alpha * along
    answer = alpha * direction

    local = apply(residual)
    loc[1] = local
    sub16w = lax.broadcasted_iota(jnp.int32, (16, 2 * nrows), 0)

    @pl.when(inner)
    def _():
        parts = local
        for z in range(quarter):
            rows = arrived[arrival(out_far + z, 1), :]
            inside = jnp.sum(lax.dot_general(
                thirds(residual, sub16), rows, (((1,), (1,)), ((), ())),
                preferred_element_type=F32,
            ), axis=0, keepdims=True)
            parts = parts + jnp.sum(jnp.dot(
                thirds(inside, sub16w), rows, preferred_element_type=F32
            ), axis=0, keepdims=True)
        loc[1] = parts

    local = loc[1]
    probe = jnp.where(sub1 == nc + 1, residual, work)
    square = 0.5 * jnp.sum(residual * residual, axis=1, keepdims=True)
    row = as_row(jnp.sum(probe * local, axis=1, keepdims=True))
    share(2, jnp.where(lane1 == 8, square, row))
    third = faces(loc.at[1], ext.at[1], 2)

    @pl.when(inner)
    def _():
        for z in range(quarter):
            base = (out_far + z) * ny + 2 * ((iy // 2 + 1) % (ny // 2))
            add(pl.ds(pl.multiple_of(base * nrows, 2 * nrows), 2 * nrows))

    for r in range(tiles):
        high[cols(r), :] = stiff[cols(r), :].astype(BF16)
    store = pltpu.make_async_copy(high, schur_ref.at[0], schur_sem)
    store.start()

    def drained(count):
        whole = outgoing.at[pl.ds(0, count)]
        pltpu.make_async_remote_copy(
            src_ref=whole, dst_ref=whole, send_sem=bsend, recv_sem=precv,
            device_id=(ix, iy, mirror), device_id_type=MESH,
        ).wait_send()

    @pl.when(outer)
    def _():
        drained(4 * group - 1)
        whole(part_out, part_send, part_recv).wait_send()
        pltpu.make_async_remote_copy(
            src_ref=passing, dst_ref=passing, send_sem=hop_send, recv_sem=hop_recv.at[0],
            device_id=(ix, iy, mirror), device_id_type=MESH,
        ).wait_send()

    @pl.when(inner)
    def _():
        drained(2 * group + team - 2)
        whole(probe_in, probe_send, probe_recv).wait_send()
        pltpu.make_async_remote_copy(
            src_ref=code_out, dst_ref=code_in, send_sem=csend, recv_sem=crecv.at[0],
            device_id=(ix, iy, mirror), device_id_type=MESH,
        ).wait_send()
        pltpu.make_async_remote_copy(
            src_ref=meta_out, dst_ref=meta_in, send_sem=msend, recv_sem=mrecv.at[0],
            device_id=(ix, iy, mirror), device_id_type=MESH,
        ).wait_send()

    for turn, copies in enumerate((first, second)):
        copies.wait_send()
        all_rows(turn).wait_send()

    third.wait_recv()
    total = gathered(2)
    g_two = as_column(total)
    norm_next = jnp.sum(jnp.where(lane1 == 8, total, 0.0), axis=1, keepdims=True)
    beta = norm_next / norm_now
    curve = (
        g_two[nc + 1 : nc + 2, :]
        + 2.0 * beta * g_two[nc : nc + 1, :]
        + beta * beta * curve_one
    )
    image = local + ext[1] + beta * image
    along = image - jnp.sum((g_two + beta * g_one) * basis, axis=0, keepdims=True)
    alpha = norm_next / curve
    ends[0] = answer + alpha * (residual + beta * direction)
    ends[1] = residual - alpha * along
    puts = [
        pltpu.make_async_copy(ends.at[i], dst, end_sem.at[i])
        for i, dst in enumerate((sol_ref, res_ref))
    ]
    for put in puts:
        put.start()

    third.wait_send()
    all_rows(2).wait_send()
    store.wait()
    for put in puts:
        put.wait()


def finish(schur_in, sol_in, res_in, schur_ref, sol_ref, res_ref, held, rows, in_sem, out_sem):
    parts = held.shape[0]
    size = held.shape[1]
    loads, stores = [], []
    for i in range(parts):
        span = pl.ds(i * size, size)
        loads.append(pltpu.make_async_copy(schur_in.at[0, span], held.at[i], in_sem.at[i]))
        stores.append(pltpu.make_async_copy(held.at[i], schur_ref.at[0, span], out_sem.at[i]))
    for i, (src, dst) in enumerate(((sol_in, sol_ref), (res_in, res_ref))):
        loads.append(pltpu.make_async_copy(src, rows.at[i], in_sem.at[parts + i]))
        stores.append(pltpu.make_async_copy(rows.at[i], dst, out_sem.at[parts + i]))
    for load in loads:
        load.start()
    for load, store in zip(loads, stores):
        load.wait()
        store.start()
    for store in stores:
        store.wait()


def solution(mesh):
    nx, ny, nz = mesh.shape["gx"], mesh.shape["gy"], mesh.shape["gz"]
    n, owners = nx * ny * nz, ny * nz
    assert ny == 4 and nz % 4 == 0

    def shards(blocks, counts, owner, kdiag, rhs, modes):
        nblk, nrows, width = blocks.shape
        folds = width // TILE // 2
        late = 2 * (ny - 2) * nz // 4
        hops = late * 3 // 2
        hbm = pl.BlockSpec(memory_space=pl.ANY)
        dma = pltpu.SemaphoreType.DMA
        made = pl.pallas_call(
            functools.partial(kernel, nx, ny, nz),
            out_shape=(
                jax.ShapeDtypeStruct((1, width, width), BF16),
                jax.ShapeDtypeStruct((1, width), F32),
                jax.ShapeDtypeStruct((1, width), F32),
            ),
            in_specs=[hbm] * 6,
            out_specs=(hbm,) * 3,
            scratch_shapes=[
                pltpu.SMEM((nblk,), jnp.int32),
                pltpu.SMEM((nblk,), jnp.int32),
                pltpu.VMEM((1, width), F32),
                pltpu.VMEM((1, width), F32),
                pltpu.VMEM((modes.shape[1], 1, width), F32),
                pltpu.VMEM((nblk, nrows, width), BF16),
                pltpu.VMEM((owners, nrows, width), BF16),
                pltpu.VMEM((owners * nrows, width), BF16),
                pltpu.VMEM((owners // 2 * nrows, width), BF16),
                pltpu.VMEM((hops, nrows, width), BF16),
                pltpu.VMEM((width, width), F32),
                pltpu.VMEM((width, width), BF16),
                pltpu.VMEM((folds, TILE, width), I16),
                pltpu.VMEM((folds, TILE, width), I16),
                pltpu.VMEM((folds + 1, 1, width), F32),
                pltpu.VMEM((folds + 1, 1, width), F32),
                pltpu.VMEM((1, width), F32),
                pltpu.VMEM((late, 1, width), F32),
                pltpu.VMEM((late, 1, width), F32),
                pltpu.VMEM((late, 1, width), F32),
                pltpu.VMEM((8, width), F32),
                pltpu.VMEM((8, width), F32),
                pltpu.VMEM((2, 1, width), F32),
                pltpu.VMEM((2, 1, width), F32),
                pltpu.VMEM((3, n, 1, 128), F32),
                pltpu.VMEM((2, 1, width), F32),
                pltpu.SemaphoreType.REGULAR, pltpu.SemaphoreType.REGULAR,
                dma, dma((5,)), dma, dma, dma, dma,
                dma, dma((hops,)),
                dma((owners // 2,)),
                dma, dma((folds,)), dma, dma((folds + 1,)),
                dma, dma, dma, dma,
                dma((3,)), dma((3,)), dma((3,)), dma((3,)), dma((2,)),
            ],
            compiler_params=pltpu.CompilerParams(
                collective_id=0, has_side_effects=True, vmem_limit_bytes=60000 * 1024
            ),
        )(counts, owner[:, 0], blocks, kdiag, rhs, jnp.transpose(modes, (1, 0, 2)))
        return pl.pallas_call(
            finish,
            out_shape=(
                jax.ShapeDtypeStruct((1, width, width), BF16),
                jax.ShapeDtypeStruct((1, width), F32),
                jax.ShapeDtypeStruct((1, width), F32),
            ),
            in_specs=[hbm] * 3,
            out_specs=(hbm,) * 3,
            scratch_shapes=[
                pltpu.VMEM((PARTS, width // PARTS, width), BF16),
                pltpu.VMEM((2, 1, width), F32),
                pltpu.SemaphoreType.DMA((PARTS + 2,)),
                pltpu.SemaphoreType.DMA((PARTS + 2,)),
            ],
        )(*made)

    every = ("gx", "gy", "gz")
    return jax.shard_map(
        shards,
        mesh=mesh,
        in_specs=(
            P(every, None, None), P(every), P(every, None),
            P(every, None), P(every, None), P(every, None, None),
        ),
        out_specs=(P(every, None, None), P(every, None), P(every, None)),
        check_vma=False,
    )
```

```python
import functools

import jax
import jax.numpy as jnp
from jax import lax
from jax.experimental import pallas as pl
from jax.experimental.pallas import tpu as pltpu
from jax.sharding import PartitionSpec as P

MESH = pl.DeviceIdType.MESH
HI = lax.Precision.HIGHEST
F32 = jnp.float32
BF16 = jnp.bfloat16
I16 = jnp.int16
TILE = 128
TOP = 32767.0
UNROLL = 64
PARTS = 8


def kernel(
    nx, ny, nz,
    counts_hbm, owner_hbm, blocks_ref, kdiag_hbm, rhs_hbm, modes_hbm,
    schur_ref, sol_ref, res_ref,
    counts_ref, owner_ref, kdiag_ref, rhs_ref, modes_ref, blk, outgoing, arrived, pool, passing, stiff, high, code_out, code_in, meta_out, meta_in,
    probe_out, probe_in, part_out, part_in,
    stack, ext0, loc, ext, slots, ends,
    y_sem, z_sem, load_sem, small_sem, schur_sem, bsend, psend, precv, hop_send, hop_recv, brecv, csend, crecv, msend, mrecv,
    probe_send, probe_recv, part_send, part_recv,
    fsend, frecv, rsend, rrecv, end_sem,
):
    n = nx * ny * nz
    quarter = nz // 4
    half = 2 * quarter
    nblk, nrows, width = blk.shape
    nc = modes_ref.shape[0]
    face = width // 8
    tiles = width // TILE
    folds = tiles // 2
    ix, iy, iz = lax.axis_index("gx"), lax.axis_index("gy"), lax.axis_index("gz")
    me = (ix * ny + iy) * nz + iz
    place = iy * nz + iz
    spot = iz * ny + iy
    side = iz // half
    off = iz % half
    seat = iy * half + off
    outer = jnp.logical_or(iz < quarter, iz >= 3 * quarter)
    inner = jnp.logical_not(outer)
    mirror = (iz + half) % nz
    near_lo = jnp.where(side == 0, quarter, half)
    far_lo = jnp.where(side == 0, half, quarter)
    group = ny * quarter
    team = ny * half

    def coords(flat):
        return (flat // (ny * nz), (flat // nz) % ny, flat % nz)

    def each_peer(act):
        if n <= UNROLL:
            steps = [
                (dx, dy, dz)
                for dx in range(nx) for dy in range(ny) for dz in range(nz)
                if dx or dy or dz
            ]
            steps.sort(key=lambda s: -(s[0] + min(s[1], ny - s[1]) + s[2]))
            for dx, dy, dz in steps:
                act(((ix + dx) % nx, (iy + dy) % ny, (iz + dz) % nz))
        else:
            def one(k, carry):
                act(coords((me + k) % n))
                return carry

            lax.fori_loop(1, n, one, 0)

    barrier = pltpu.get_barrier_semaphore()
    x_line = [((ix + d) % nx, iy, iz) for d in range(1, nx)]
    y_line = [(ix, (iy + d) % ny, iz) for d in range(1, ny)]
    z_line = [(ix, iy, (iz + d) % nz) for d in range(1, nz)]

    def tell(sem, line):
        for device in line:
            pl.semaphore_signal(sem, inc=1, device_id=device, device_id_type=MESH)

    tell(barrier, z_line + y_line + x_line)
    smalls = [
        pltpu.make_async_copy(src, dst, small_sem.at[i])
        for i, (src, dst) in enumerate((
            (rhs_hbm, rhs_ref), (modes_hbm, modes_ref), (owner_hbm, owner_ref),
            (counts_hbm, counts_ref), (kdiag_hbm, kdiag_ref),
        ))
    ]
    for small in smalls:
        small.start()
    load = pltpu.make_async_copy(blocks_ref, blk, load_sem)
    load.start()
    stack[...] = jnp.zeros_like(stack)
    for small in smalls:
        small.wait()
    for i in range(nc):
        stack[i : i + 1, :] = modes_ref[i]
    stack[nc : nc + 1, :] = rhs_ref[...]
    pl.semaphore_wait(barrier, nx + ny + nz - 3)
    tell(y_sem, y_line)

    next_x, prev_x = ((ix + 1) % nx, iy, iz), ((ix + nx - 1) % nx, iy, iz)
    next_y, prev_y = (ix, (iy + 1) % ny, iz), (ix, (iy + ny - 1) % ny, iz)
    next_z, prev_z = (ix, iy, (iz + 1) % nz), (ix, iy, (iz + nz - 1) % nz)
    plan = (
        (4, 6, 2, next_z), (6, 4, 2, prev_z),
        (2, 3, 1, next_y), (3, 2, 1, prev_y),
        (0, 1, 1, next_x), (1, 0, 1, prev_x),
    )

    def faces(src, dst, turn):
        for mine, theirs, wide, device in plan:
            pltpu.make_async_remote_copy(
                src_ref=src.at[:, mine * face : (mine + wide) * face],
                dst_ref=dst.at[:, theirs * face : (theirs + wide) * face],
                send_sem=fsend.at[turn],
                recv_sem=frecv.at[turn],
                device_id=device,
                device_id_type=MESH,
            ).start()
        return pltpu.make_async_remote_copy(
            src_ref=src, dst_ref=dst, send_sem=fsend.at[turn], recv_sem=frecv.at[turn],
            device_id=next_x, device_id_type=MESH,
        )

    def share(turn, row):
        slots[turn, me] = row
        each_peer(
            lambda device: pltpu.make_async_remote_copy(
                src_ref=slots.at[turn, me],
                dst_ref=slots.at[turn, me],
                send_sem=rsend.at[turn],
                recv_sem=rrecv.at[turn],
                device_id=device,
                device_id_type=MESH,
            ).start()
        )

    def all_rows(turn):
        return pltpu.make_async_remote_copy(
            src_ref=slots.at[turn, pl.ds(0, n - 1)],
            dst_ref=slots.at[turn, pl.ds(0, n - 1)],
            send_sem=rsend.at[turn],
            recv_sem=rrecv.at[turn],
            device_id=next_x,
            device_id_type=MESH,
        )

    def gathered(turn):
        all_rows(turn).wait_recv()
        return jnp.sum(slots[turn], axis=0)

    first = faces(stack, ext0, 0)
    load.wait()

    owned = [owner_ref[b] for b in range(nblk)]
    counted = [counts_ref[b] for b in range(nblk)]
    rowid = lax.broadcasted_iota(jnp.int32, (nrows, width), 0)

    def chosen(target):
        which = jnp.int32(0)
        count = jnp.int32(0)
        for b in range(nblk):
            same = owned[b] == target
            which = jnp.where(same, b, which)
            count = jnp.where(same, counted[b], count)
        value = blk[which]
        return jnp.where(rowid < count, value, jnp.zeros_like(value))

    def block_rows(at):
        return pl.ds(pl.multiple_of(at * nrows, nrows), nrows)

    def block_copy(slot, ty, tz, src):
        return pltpu.make_async_remote_copy(
            src_ref=outgoing.at[slot],
            dst_ref=arrived.at[block_rows(src), :],
            send_sem=bsend,
            recv_sem=brecv.at[src // 2],
            device_id=(ix, ty, tz),
            device_id_type=MESH,
        )

    def pool_copy(slot, ty, tz, src):
        return pltpu.make_async_remote_copy(
            src_ref=outgoing.at[slot],
            dst_ref=pool.at[block_rows(src), :],
            send_sem=bsend,
            recv_sem=precv,
            device_id=(ix, ty, tz),
            device_id_type=MESH,
        )

    def push_pool(t, carry):
        ty = (iy + t // quarter) % ny
        tz = near_lo + (off + t) % quarter
        value = chosen(ty * nz + (tz + half) % nz)
        itself = jnp.logical_and(ty == iy, tz == iz)

        @pl.when(itself)
        def _():
            pool[block_rows(seat), :] = value

        @pl.when(jnp.logical_not(itself))
        def _():
            outgoing[t] = value
            pool_copy(t, ty, tz, seat).start()

        return carry

    def push_far(t, carry):
        ty = (iy + t // quarter) % ny
        tz = far_lo + (off + t) % quarter
        outgoing[group + t] = chosen(ty * nz + tz)
        block_copy(group + t, ty, tz, spot).start()
        return carry

    def push_own(t, carry):
        ty = (iy + (t + 1) // half) % ny
        tz = side * half + (off + t + 1) % half
        outgoing[2 * group + t] = chosen(ty * nz + tz)
        block_copy(2 * group + t, ty, tz, spot).start()
        return carry

    def push_both(t, carry):
        push_far(t, carry)
        return push_pool(t, carry)

    def swing(u):
        return 2 * ((iy // 2 + u // 2) % (ny // 2)) + (iy + u) % 2

    direct = 2 * quarter
    hops = group - direct
    kinds = ((near_lo, half, 0), (near_lo, 0, 2 * group), (far_lo, 0, group))

    def fill(kind, t):
        lo, shift, slot = kinds[kind]
        ty, tz = swing(t // quarter), lo + (off + t) % quarter
        outgoing[slot + t] = chosen(ty * nz + (tz + shift) % nz)
        return slot + t, ty, tz

    def push_direct(kind):
        def one(t, carry):
            slot, ty, tz = fill(kind, t)
            if kind:
                block_copy(slot, ty, tz, spot).start()
            else:
                pool_copy(slot, ty, tz, seat).start()
            return carry

        return one

    def hop_copy(slot, s, peer):
        return pltpu.make_async_remote_copy(
            src_ref=outgoing.at[slot], dst_ref=passing.at[s],
            send_sem=bsend, recv_sem=hop_recv.at[s],
            device_id=(ix, peer, iz), device_id_type=MESH,
        )

    def push_hop(kind):
        def one(s, carry):
            slot, ty, tz = fill(kind, direct + s)
            hop_copy(slot, kind * hops + s, 2 * (ty // 2) + iy % 2).start()
            return carry

        return one

    def pass_on(kind):
        def one(s, carry):
            t = direct + s
            turn = t // quarter // 2
            sy = 2 * ((iy // 2 + ny // 2 - turn) % (ny // 2)) + iy % 2
            ty = 2 * (iy // 2) + (iy + t // quarter) % 2
            tz = kinds[kind][0] + (off + t) % quarter
            if kind:
                src = iz * ny + sy
                dst, sem = arrived.at[block_rows(src), :], brecv.at[src // 2]
            else:
                hop_copy(0, s, iy).wait_recv()
                dst, sem = pool.at[block_rows(sy * half + off), :], precv
            pltpu.make_async_remote_copy(
                src_ref=passing.at[kind * hops + s], dst_ref=dst,
                send_sem=hop_send, recv_sem=sem,
                device_id=(ix, ty, tz), device_id_type=MESH,
            ).start()
            return carry

        return one

    out_lo = jnp.where(side == 0, 0, 3 * quarter)
    out_near, out_far = out_lo, 3 * quarter - out_lo
    mine_lo = near_lo

    def push_out(t, carry):
        ty = (iy + (t + 1) // quarter) % ny
        tz = out_lo + (iz - out_lo + t + 1) % quarter
        outgoing[3 * group + t] = chosen(ty * nz + tz)
        block_copy(3 * group + t, ty, tz, spot).start()
        return carry

    @pl.when(outer)
    def _():
        lax.fori_loop(0, hops, push_hop(0), 0)
        lax.fori_loop(0, quarter, push_direct(0), 0)

    @pl.when(inner)
    def _():
        lax.fori_loop(0, quarter, push_both, 0)

    lane = lax.broadcasted_iota(jnp.int32, (8, 128), 1)
    sub = lax.broadcasted_iota(jnp.int32, (8, 128), 0)
    sub1 = lax.broadcasted_iota(jnp.int32, (8, 1), 0)
    lane1 = lax.broadcasted_iota(jnp.int32, (1, 128), 1)

    pl.semaphore_wait(y_sem, ny - 1)
    tell(z_sem, z_line)
    first.wait_recv()
    pl.semaphore_wait(z_sem, nz - 1)
    work = stack[...] + ext0[...]
    tall = jnp.concatenate([work] * 16, axis=0)
    pairs = 0.5 * lax.dot_general(
        work, tall, (((1,), (1,)), ((), ())), precision=HI, preferred_element_type=F32
    )
    share(0, jnp.sum(jnp.where(lane // 8 == sub, pairs, 0.0), axis=0, keepdims=True))

    @pl.when(inner)
    def _():
        lax.fori_loop(quarter, group, push_both, 0)
        lax.fori_loop(0, team - 1, push_own, 0)

    @pl.when(outer)
    def _():
        lax.fori_loop(quarter, direct, push_direct(0), 0)
        lax.fori_loop(0, hops, push_hop(1), 0)
        lax.fori_loop(0, hops, push_hop(2), 0)
        lax.fori_loop(0, group - 1, push_out, 0)
        lax.fori_loop(0, quarter, pass_on(0), 0)
        lax.fori_loop(quarter, direct, pass_on(0), 0)
        lax.fori_loop(0, quarter, push_direct(2), 0)
        lax.fori_loop(quarter, direct, push_direct(2), 0)
        lax.fori_loop(0, quarter, push_direct(1), 0)
        lax.fori_loop(quarter, direct, push_direct(1), 0)

    arrived[block_rows(spot), :] = chosen(place)

    diag_r = lax.broadcasted_iota(jnp.int32, (TILE, width), 0)
    diag_c = lax.broadcasted_iota(jnp.int32, (TILE, width), 1)
    for r in range(tiles):
        stiff[r * TILE : (r + 1) * TILE, :] = jnp.where(
            diag_r + r * TILE == diag_c, kdiag_ref[...], 0.0
        )

    tile_r = lax.broadcasted_iota(jnp.int32, (TILE, TILE), 0)
    tile_c = lax.broadcasted_iota(jnp.int32, (TILE, TILE), 1)
    above, below, level = tile_r < tile_c, tile_r > tile_c, tile_r == tile_c

    def cols(k):
        return slice(k * TILE, (k + 1) * TILE)

    def code_copy(a):
        return pltpu.make_async_remote_copy(
            src_ref=code_out.at[a], dst_ref=code_in.at[a],
            send_sem=csend, recv_sem=crecv.at[a],
            device_id=(ix, iy, mirror), device_id_type=MESH,
        )

    def meta_copy(a):
        return pltpu.make_async_remote_copy(
            src_ref=meta_out.at[a], dst_ref=meta_in.at[a],
            send_sem=msend, recv_sem=mrecv.at[a],
            device_id=(ix, iy, mirror), device_id_type=MESH,
        )

    total = gathered(0)
    spread = jnp.where(lane // 8 == sub, total, 0.0)
    fold_r = lax.broadcasted_iota(jnp.int32, (128, 128), 0)
    fold_c = lax.broadcasted_iota(jnp.int32, (128, 128), 1)
    fold = jnp.where(fold_r % 8 == fold_c, 1.0, 0.0).astype(F32)
    coarse = jnp.dot(spread, fold, precision=HI, preferred_element_type=F32)
    for k in range(nc):
        ratio = jnp.where(sub1 > k, coarse[:, k : k + 1] / coarse[k : k + 1, k : k + 1], 0.0)
        coarse_row = coarse[k : k + 1, :]
        work_row = work[k : k + 1, :]
        coarse = coarse - ratio * coarse_row
        work = work - ratio * work_row
    diag = jnp.sum(jnp.where(lane == sub, coarse, 0.0), axis=1, keepdims=True)
    norm_now = diag[nc : nc + 1, :]
    work = work * jnp.where(sub1 < nc, 1.0 / jnp.sqrt(jnp.where(sub1 < nc, diag, 1.0)), 1.0)
    direction = work[nc : nc + 1, :]
    basis = jnp.where(sub1 < nc, work, 0.0)

    probe_out[...] = direction
    late = 2 * hops

    def probe_copy(k, c, z):
        base, away = ((out_near, near_lo), (out_far, far_lo))[k]
        tz = base + z
        ty = 2 * (iy // 2) + c
        j = (iy + c) % 2
        far_off = tz % half
        r = (iz - mine_lo + quarter - far_off % quarter) % quarter
        return pltpu.make_async_remote_copy(
            src_ref=probe_out,
            dst_ref=probe_in.at[k * hops + j * quarter + r],
            send_sem=probe_send, recv_sem=probe_recv,
            device_id=(ix, ty, tz), device_id_type=MESH,
        )

    def whole(ref, send, recv):
        return pltpu.make_async_remote_copy(
            src_ref=ref, dst_ref=ref, send_sem=send, recv_sem=recv,
            device_id=(ix, iy, mirror), device_id_type=MESH,
        )

    sub16 = lax.broadcasted_iota(jnp.int32, (16, width), 0)
    sub16t = lax.broadcasted_iota(jnp.int32, (16, nrows), 0)

    def thirds(row, which):
        x = row.astype(BF16).astype(F32)
        y = (row - x).astype(BF16).astype(F32)
        z = row - x - y
        return jnp.where(
            which == 0, x, jnp.where(which == 1, y, jnp.where(which == 2, z, 0.0))
        ).astype(BF16)

    @pl.when(inner)
    def _():
        for k in range(2):
            for c in range(2):
                for z in range(quarter):
                    probe_copy(k, c, z).start()

    @pl.when(outer)
    def _():
        def landed(s, carry):
            hop_copy(0, hops + s, iy).wait_recv()
            return carry

        lax.fori_loop(0, late, landed, 0)
        whole(probe_in, probe_send, probe_recv).wait_recv()

        def part(s, carry):
            rows = passing[hops + s]
            inside = jnp.sum(lax.dot_general(
                thirds(probe_in[s], sub16), rows, (((1,), (1,)), ((), ())),
                preferred_element_type=F32,
            ), axis=0, keepdims=True)
            part_out[s] = jnp.sum(jnp.dot(
                thirds(inside, sub16t), rows, preferred_element_type=F32
            ), axis=0, keepdims=True)
            k = s // hops
            t = direct + s % hops
            j = t // quarter - 2
            tz = jnp.where(k == 0, near_lo, far_lo) + (off + t) % quarter
            pltpu.make_async_remote_copy(
                src_ref=part_out.at[s],
                dst_ref=part_in.at[k * hops + j * quarter + iz - out_lo],
                send_sem=part_send, recv_sem=part_recv,
                device_id=(ix, 2 * (iy // 2) + (iy + j) % 2, tz), device_id_type=MESH,
            ).start()
            return carry

        lax.fori_loop(0, late, part, 0)
        lax.fori_loop(0, hops, pass_on(1), 0)
        lax.fori_loop(0, quarter, pass_on(2), 0)

    @pl.when(inner)
    def _():
        pltpu.make_async_remote_copy(
            src_ref=pool.at[pl.ds(0, (team - 1) * nrows), :],
            dst_ref=pool.at[pl.ds(0, (team - 1) * nrows), :],
            send_sem=psend, recv_sem=precv,
            device_id=(ix, iy, mirror), device_id_type=MESH,
        ).wait_recv()

        def strip(k):
            return lax.dot_general(
                pool[:, cols(k)], pool[:, k * TILE :], (((0,), (0,)), ((), ())),
                preferred_element_type=F32,
            )

        for a in range(folds):
            b = tiles - 1 - a
            upper, lower = strip(a), strip(b)
            at_a, at_b = upper[:, :TILE], lower[:, :TILE]
            for k, corner in ((a, at_a), (b, at_b)):
                meta_out[folds, :, cols(k)] = jnp.sum(
                    jnp.where(level, corner, 0.0), axis=0, keepdims=True
                )
            corners = jnp.where(above, at_a, jnp.where(below, at_b, 0.0))
            parts = [upper[:, TILE:]]
            if a:
                parts.append(lower[:, TILE:])
            value = jnp.concatenate(parts + [corners], axis=1)
            most = jnp.max(jnp.abs(value), axis=0, keepdims=True)
            scale = TOP / jnp.maximum(most, 1e-30)
            code_out[a] = jnp.round(value * scale).astype(jnp.int32).astype(I16)
            meta_out[a] = most * (1.0 / TOP)
            code_copy(a).start()
            meta_copy(a).start()
        meta_copy(folds).start()

    def arrival(sz, chip):
        base = sz * ny + 2 * ((iy // 2 + chip) % (ny // 2))
        remote = pltpu.make_async_remote_copy(
            src_ref=outgoing.at[0],
            dst_ref=arrived.at[block_rows(base), :],
            send_sem=bsend, recv_sem=brecv.at[base // 2],
            device_id=(ix, iy, mirror), device_id_type=MESH,
        )
        pair = pl.ds(pl.multiple_of(base * nrows, 2 * nrows), 2 * nrows)
        both = pltpu.make_async_remote_copy(
            src_ref=arrived.at[pair, :], dst_ref=arrived.at[pair, :],
            send_sem=bsend, recv_sem=brecv.at[base // 2],
            device_id=(ix, iy, mirror), device_id_type=MESH,
        )
        mine = base // 2 == spot // 2

        @pl.when(mine)
        def _():
            remote.wait_recv()

        @pl.when(jnp.logical_not(mine))
        def _():
            both.wait_recv()

        return pair

    def add(pair):
        rows = arrived[pair, :]
        for c in range(width // 256):
            span = slice(c * 256, (c + 1) * 256)
            stiff[:, span] += lax.dot_general(
                rows, rows[:, span], (((0,), (0,)), ((), ())), preferred_element_type=F32
            )

    def take(sz, chip):
        add(arrival(sz, chip))

    chips = ny // 2

    def takes(lo, first_chip, last_chip):
        def one(u, carry):
            count = last_chip - first_chip
            take(lo + u // count, first_chip + u % count)
            return carry

        lax.fori_loop(0, quarter * (last_chip - first_chip), one, 0)

    @pl.when(inner)
    def _():
        takes(near_lo, 0, chips)
        takes(far_lo, 0, chips)
        takes(out_far, 0, 1)
        takes(out_near, 0, 1)

    @pl.when(outer)
    def _():
        takes(out_near, 0, chips)
        takes(near_lo, 0, chips)

    @pl.when(outer)
    def _():
        for a in range(folds):
            b = tiles - 1 - a
            code_copy(a).wait_recv()
            meta_copy(a).wait_recv()
            value = code_in[a].astype(jnp.int32).astype(F32) * meta_in[a]
            spots = [(a, a + j) for j in range(1, tiles - a)]
            spots += [(b, b + j) for j in range(1, tiles - b)]
            for at, (r, c) in enumerate(spots):
                piece = value[:, cols(at)]
                stiff[cols(r), cols(c)] += piece
                stiff[cols(c), cols(r)] += piece.T
            corners = value[:, cols(tiles - 1)]
            turned = corners.T
            stiff[cols(a), cols(a)] += jnp.where(
                above, corners, jnp.where(below, turned, 0.0)
            )
            stiff[cols(b), cols(b)] += jnp.where(
                below, corners, jnp.where(above, turned, 0.0)
            )
        meta_copy(folds).wait_recv()
        for r in range(tiles):
            stiff[cols(r), cols(r)] += jnp.where(level, meta_in[folds, :, cols(r)], 0.0)

    def apply(vector):
        sums = [jnp.zeros((8, TILE), F32) for _ in range(tiles)]
        for k in range(tiles):
            column = jnp.broadcast_to(vector[:, cols(k)], (TILE, TILE)).T
            for c in range(tiles):
                product = stiff[cols(k), cols(c)] * column
                sums[c] = sums[c] + jnp.sum(product.reshape(TILE // 8, 8, TILE), axis=0)
        return jnp.concatenate([jnp.sum(s, axis=0, keepdims=True) for s in sums], axis=1)

    def as_row(column):
        return jnp.sum(jnp.where(lane == sub, column, 0.0), axis=0, keepdims=True)

    def as_column(row):
        return jnp.sum(jnp.where(lane == sub, row, 0.0), axis=1, keepdims=True)

    local = apply(direction)
    loc[0] = local

    @pl.when(inner)
    def _():
        whole(part_in, part_send, part_recv).wait_recv()
        loc[0] = local + jnp.sum(part_in[...], axis=0)

    local = loc[0]
    share(1, as_row(jnp.sum(work * local, axis=1, keepdims=True)))
    second = faces(loc.at[0], ext.at[0], 1)

    @pl.when(outer)
    def _():
        lax.fori_loop(quarter, hops, pass_on(2), 0)

    @pl.when(inner)
    def _():
        takes(out_near, 1, chips)

    second.wait_recv()
    image = local + ext[0]
    g_one = as_column(gathered(1))
    curve_one = g_one[nc : nc + 1, :]
    alpha = norm_now / curve_one
    along = image - jnp.sum(g_one * basis, axis=0, keepdims=True)
    residual = direction - alpha * along
    answer = alpha * direction

    local = apply(residual)
    loc[1] = local
    sub16w = lax.broadcasted_iota(jnp.int32, (16, 2 * nrows), 0)

    @pl.when(inner)
    def _():
        parts = local
        for z in range(quarter):
            rows = arrived[arrival(out_far + z, 1), :]
            inside = jnp.sum(lax.dot_general(
                thirds(residual, sub16), rows, (((1,), (1,)), ((), ())),
                preferred_element_type=F32,
            ), axis=0, keepdims=True)
            parts = parts + jnp.sum(jnp.dot(
                thirds(inside, sub16w), rows, preferred_element_type=F32
            ), axis=0, keepdims=True)
        loc[1] = parts

    local = loc[1]
    probe = jnp.where(sub1 == nc + 1, residual, work)
    square = 0.5 * jnp.sum(residual * residual, axis=1, keepdims=True)
    row = as_row(jnp.sum(probe * local, axis=1, keepdims=True))
    share(2, jnp.where(lane1 == 8, square, row))
    third = faces(loc.at[1], ext.at[1], 2)

    @pl.when(inner)
    def _():
        for z in range(quarter):
            base = (out_far + z) * ny + 2 * ((iy // 2 + 1) % (ny // 2))
            add(pl.ds(pl.multiple_of(base * nrows, 2 * nrows), 2 * nrows))

    for r in range(tiles):
        high[cols(r), :] = stiff[cols(r), :].astype(BF16)
    store = pltpu.make_async_copy(high, schur_ref.at[0], schur_sem)
    store.start()

    def drained(count):
        whole = outgoing.at[pl.ds(0, count)]
        pltpu.make_async_remote_copy(
            src_ref=whole, dst_ref=whole, send_sem=bsend, recv_sem=precv,
            device_id=(ix, iy, mirror), device_id_type=MESH,
        ).wait_send()

    @pl.when(outer)
    def _():
        drained(4 * group - 1)
        whole(part_out, part_send, part_recv).wait_send()
        pltpu.make_async_remote_copy(
            src_ref=passing, dst_ref=passing, send_sem=hop_send, recv_sem=hop_recv.at[0],
            device_id=(ix, iy, mirror), device_id_type=MESH,
        ).wait_send()

    @pl.when(inner)
    def _():
        drained(2 * group + team - 2)
        whole(probe_in, probe_send, probe_recv).wait_send()
        pltpu.make_async_remote_copy(
            src_ref=code_out, dst_ref=code_in, send_sem=csend, recv_sem=crecv.at[0],
            device_id=(ix, iy, mirror), device_id_type=MESH,
        ).wait_send()
        pltpu.make_async_remote_copy(
            src_ref=meta_out, dst_ref=meta_in, send_sem=msend, recv_sem=mrecv.at[0],
            device_id=(ix, iy, mirror), device_id_type=MESH,
        ).wait_send()

    for turn, copies in enumerate((first, second)):
        copies.wait_send()
        all_rows(turn).wait_send()

    third.wait_recv()
    total = gathered(2)
    g_two = as_column(total)
    norm_next = jnp.sum(jnp.where(lane1 == 8, total, 0.0), axis=1, keepdims=True)
    beta = norm_next / norm_now
    curve = (
        g_two[nc + 1 : nc + 2, :]
        + 2.0 * beta * g_two[nc : nc + 1, :]
        + beta * beta * curve_one
    )
    image = local + ext[1] + beta * image
    along = image - jnp.sum((g_two + beta * g_one) * basis, axis=0, keepdims=True)
    alpha = norm_next / curve
    ends[0] = answer + alpha * (residual + beta * direction)
    ends[1] = residual - alpha * along
    puts = [
        pltpu.make_async_copy(ends.at[i], dst, end_sem.at[i])
        for i, dst in enumerate((sol_ref, res_ref))
    ]
    for put in puts:
        put.start()

    third.wait_send()
    all_rows(2).wait_send()
    store.wait()
    for put in puts:
        put.wait()


def finish(schur_in, sol_in, res_in, schur_ref, sol_ref, res_ref, held, rows, in_sem, out_sem):
    parts = held.shape[0]
    size = held.shape[1]
    loads, stores = [], []
    for i in range(parts):
        span = pl.ds(i * size, size)
        loads.append(pltpu.make_async_copy(schur_in.at[0, span], held.at[i], in_sem.at[i]))
        stores.append(pltpu.make_async_copy(held.at[i], schur_ref.at[0, span], out_sem.at[i]))
    for i, (src, dst) in enumerate(((sol_in, sol_ref), (res_in, res_ref))):
        loads.append(pltpu.make_async_copy(src, rows.at[i], in_sem.at[parts + i]))
        stores.append(pltpu.make_async_copy(rows.at[i], dst, out_sem.at[parts + i]))
    for load in loads:
        load.start()
    for load, store in zip(loads, stores):
        load.wait()
        store.start()
    for store in stores:
        store.wait()


def solution(mesh):
    nx, ny, nz = mesh.shape["gx"], mesh.shape["gy"], mesh.shape["gz"]
    n, owners = nx * ny * nz, ny * nz
    assert ny == 4 and nz % 4 == 0

    def shards(blocks, counts, owner, kdiag, rhs, modes):
        nblk, nrows, width = blocks.shape
        folds = width // TILE // 2
        late = 2 * (ny - 2) * nz // 4
        hops = late * 3 // 2
        hbm = pl.BlockSpec(memory_space=pl.ANY)
        dma = pltpu.SemaphoreType.DMA
        made = pl.pallas_call(
            functools.partial(kernel, nx, ny, nz),
            out_shape=(
                jax.ShapeDtypeStruct((1, width, width), BF16),
                jax.ShapeDtypeStruct((1, width), F32),
                jax.ShapeDtypeStruct((1, width), F32),
            ),
            in_specs=[hbm] * 6,
            out_specs=(hbm,) * 3,
            scratch_shapes=[
                pltpu.SMEM((nblk,), jnp.int32),
                pltpu.SMEM((nblk,), jnp.int32),
                pltpu.VMEM((1, width), F32),
                pltpu.VMEM((1, width), F32),
                pltpu.VMEM((modes.shape[1], 1, width), F32),
                pltpu.VMEM((nblk, nrows, width), BF16),
                pltpu.VMEM((owners, nrows, width), BF16),
                pltpu.VMEM((owners * nrows, width), BF16),
                pltpu.VMEM((owners // 2 * nrows, width), BF16),
                pltpu.VMEM((hops, nrows, width), BF16),
                pltpu.VMEM((width, width), F32),
                pltpu.VMEM((width, width), BF16),
                pltpu.VMEM((folds, TILE, width), I16),
                pltpu.VMEM((folds, TILE, width), I16),
                pltpu.VMEM((folds + 1, 1, width), F32),
                pltpu.VMEM((folds + 1, 1, width), F32),
                pltpu.VMEM((1, width), F32),
                pltpu.VMEM((late, 1, width), F32),
                pltpu.VMEM((late, 1, width), F32),
                pltpu.VMEM((late, 1, width), F32),
                pltpu.VMEM((8, width), F32),
                pltpu.VMEM((8, width), F32),
                pltpu.VMEM((2, 1, width), F32),
                pltpu.VMEM((2, 1, width), F32),
                pltpu.VMEM((3, n, 1, 128), F32),
                pltpu.VMEM((2, 1, width), F32),
                pltpu.SemaphoreType.REGULAR, pltpu.SemaphoreType.REGULAR,
                dma, dma((5,)), dma, dma, dma, dma,
                dma, dma((hops,)),
                dma((owners // 2,)),
                dma, dma((folds,)), dma, dma((folds + 1,)),
                dma, dma, dma, dma,
                dma((3,)), dma((3,)), dma((3,)), dma((3,)), dma((2,)),
            ],
            compiler_params=pltpu.CompilerParams(
                collective_id=0, has_side_effects=True, vmem_limit_bytes=60000 * 1024
            ),
        )(counts, owner[:, 0], blocks, kdiag, rhs, jnp.transpose(modes, (1, 0, 2)))
        return pl.pallas_call(
            finish,
            out_shape=(
                jax.ShapeDtypeStruct((1, width, width), BF16),
                jax.ShapeDtypeStruct((1, width), F32),
                jax.ShapeDtypeStruct((1, width), F32),
            ),
            in_specs=[hbm] * 3,
            out_specs=(hbm,) * 3,
            scratch_shapes=[
                pltpu.VMEM((PARTS, width // PARTS, width), BF16),
                pltpu.VMEM((2, 1, width), F32),
                pltpu.SemaphoreType.DMA((PARTS + 2,)),
                pltpu.SemaphoreType.DMA((PARTS + 2,)),
            ],
        )(*made)

    every = ("gx", "gy", "gz")
    return jax.shard_map(
        shards,
        mesh=mesh,
        in_specs=(
            P(every, None, None), P(every), P(every, None),
            P(every, None), P(every, None), P(every, None, None),
        ),
        out_specs=(P(every, None, None), P(every, None), P(every, None)),
        check_vma=False,
    )
```
